64 devices in a mesh: graph: 4 (over x, y), nodes: 16 (over z, core).
Axes of the slice: x: 2, y: 2, z: 8, core: 2. Of those that a mesh axis runs over, the one named last changes fastest.
The devices are a block of a 4x4x8 slice.
Arguments:
- node_feats: bfloat16 [131072, 200], P(('graph', 'nodes')), parts along dimension 0
- a_int: bfloat16 [131072, 2048], P(('graph', 'nodes')), parts along dimension 0
- a_halo: bfloat16 [131072, 1024], P(('graph', 'nodes')), parts along dimension 0
- send_idx: int32 [256, 256], P(('graph', 'nodes')), parts along dimension 0
- w_first: bfloat16 [200, 512], replicated
- w_second: bfloat16 [512, 107], replicated
- grad_out: bfloat16 [131072, 107], P(('graph', 'nodes')), parts along dimension 0
Outputs:
- output 1: float32 [800, 512], P('graph'), parts along dimension 0
- output 2: float32 [2048, 107], P('graph'), parts along dimension 0
- output 3: float32 [131072, 200], P(('graph', 'nodes')), parts along dimension 0
There are 4 independent parts. The reference program is written for one: setup_inputs(seed, part) draws one part's arguments, and reference() takes and returns one part's arrays. A program takes and returns all parts, laid end to end along the dimension named above; an argument that names none is the same for every part.
All inputs are finite; a program needn't handle non-finite values.
Results may differ from the reference program's by a relative error of at most 0.00607032.
Values are sent between devices in bfloat16 or wider.
A program may use at most 768 MiB of HBM per device.

```python
import jax
import jax.numpy as jnp
from jax import lax

GROUP_SIZE = 16
NODES_DEV = 2048
HALO_SLOTS = 256
MAX_HOPS = 2
FEAT_IN = 200
HIDDEN = 512
CLASSES = 107
INNER_DEGREE = 16
HALO_DEGREE = 4

NUM_LINKS = 2 * MAX_HOPS
OFFSETS = [(link // 2 + 1) * (1 - 2 * (link % 2)) for link in range(NUM_LINKS)]


def draw_graph(key):
    key_count, key_order, key_blocks = jax.random.split(key, 3)
    window = 2 * HALO_SLOTS
    counts = jax.random.randint(key_count, (GROUP_SIZE, NUM_LINKS), HALO_SLOTS // 4, HALO_SLOTS + 1)
    counts = counts.at[0, 0].set(HALO_SLOTS)
    scores = jax.random.randint(key_order, (GROUP_SIZE, NUM_LINKS, window), 0, 65536) * window + jnp.arange(window)
    slot_order = jnp.argsort(scores, axis=-1)[:, :, :HALO_SLOTS]
    upward = jnp.array([offset > 0 for offset in OFFSETS])
    window_base = jnp.where(upward, NODES_DEV - window, 0)
    slot_pos = jnp.arange(HALO_SLOTS)
    used_slot = slot_pos[None, None, :] < counts[:, :, None]
    send_idx = jnp.where(used_slot, slot_order + window_base[None, :, None], 0).astype(jnp.int32)
    recv_counts = jnp.stack([jnp.roll(counts[:, link], OFFSETS[link]) for link in range(NUM_LINKS)], axis=1)
    row_pos = jnp.arange(NODES_DEV)
    low_half = row_pos < NODES_DEV // 2
    row_ok = jnp.where(upward[None, :], low_half[:, None], jnp.logical_not(low_half)[:, None])

    def one_device(inputs):
        dev_key, recv_count = inputs
        key_mask, key_inner, key_hmask, key_halo = jax.random.split(dev_key, 4)
        inner_mask = jnp.logical_or(jax.random.randint(key_mask, (NODES_DEV, NODES_DEV), 0, NODES_DEV) < INNER_DEGREE, row_pos[:, None] == row_pos[None, :])
        col_ok = slot_pos[None, :] < recv_count[:, None]
        halo_mask = (jax.random.randint(key_hmask, (NODES_DEV, NUM_LINKS, HALO_SLOTS), 0, HALO_SLOTS) < HALO_DEGREE) & row_ok[:, :, None] & col_ok[None, :, :]
        inner_w = jnp.where(inner_mask, jax.random.uniform(key_inner, (NODES_DEV, NODES_DEV), jnp.float32, 0.5, 1.5), 0.0)
        halo_w = jnp.where(halo_mask, jax.random.uniform(key_halo, (NODES_DEV, NUM_LINKS, HALO_SLOTS), jnp.float32, 0.5, 1.5), 0.0)
        degree = jnp.sum(inner_mask, axis=1) + jnp.sum(halo_mask, axis=(1, 2))
        row_scale = lax.rsqrt(degree.astype(jnp.float32))
        inner_adj = (inner_w * row_scale[:, None]).astype(jnp.bfloat16)
        halo_adj = (halo_w * row_scale[:, None, None]).reshape(NODES_DEV, NUM_LINKS * HALO_SLOTS).astype(jnp.bfloat16)
        return inner_adj, halo_adj

    inner_adj, halo_adj = lax.map(one_device, (jax.random.split(key_blocks, GROUP_SIZE), recv_counts))
    return (inner_adj.reshape(GROUP_SIZE * NODES_DEV, NODES_DEV), halo_adj.reshape(GROUP_SIZE * NODES_DEV, NUM_LINKS * HALO_SLOTS), send_idx.reshape(GROUP_SIZE * NUM_LINKS, HALO_SLOTS))


def setup_inputs(seed: int = 0, part: int = 0) -> dict:
    root_key = jax.random.key(seed)
    shared_key, parts_key = jax.random.split(root_key)
    key_first, key_second = jax.random.split(shared_key)
    part_key = jax.random.fold_in(parts_key, part)
    key_feats, key_grad, key_graph = jax.random.split(part_key, 3)
    rows_total = GROUP_SIZE * NODES_DEV
    node_feats = jax.random.normal(key_feats, (rows_total, FEAT_IN), jnp.float32).astype(jnp.bfloat16)
    grad_out = jax.random.normal(key_grad, (rows_total, CLASSES), jnp.float32).astype(jnp.bfloat16)
    w_first = (jax.random.normal(key_first, (FEAT_IN, HIDDEN), jnp.float32) * FEAT_IN ** -0.5).astype(jnp.bfloat16)
    w_second = (jax.random.normal(key_second, (HIDDEN, CLASSES), jnp.float32) * HIDDEN ** -0.5).astype(jnp.bfloat16)
    a_int, a_halo, send_idx = draw_graph(key_graph)
    return {"node_feats": node_feats, "a_int": a_int, "a_halo": a_halo, "send_idx": send_idx, "w_first": w_first, "w_second": w_second, "grad_out": grad_out}


def aggregate(a_int, a_halo, features, send_idx):
    feat_width = features.shape[-1]
    local_rows = features.reshape(GROUP_SIZE, NODES_DEV, feat_width)
    send_plan = send_idx.reshape(GROUP_SIZE, NUM_LINKS * HALO_SLOTS)
    sent_rows = jax.vmap(lambda rows_dev, plan_dev: jnp.take(rows_dev, plan_dev, axis=0))(local_rows, send_plan)
    sent_rows = sent_rows.reshape(GROUP_SIZE, NUM_LINKS, HALO_SLOTS, feat_width)
    halo_rows = jnp.stack([jnp.roll(sent_rows[:, link], OFFSETS[link], axis=0) for link in range(NUM_LINKS)], axis=1)
    halo_rows = halo_rows.reshape(GROUP_SIZE, NUM_LINKS * HALO_SLOTS, feat_width)
    blocks = (a_int.reshape(GROUP_SIZE, NODES_DEV, NODES_DEV), a_halo.reshape(GROUP_SIZE, NODES_DEV, NUM_LINKS * HALO_SLOTS), local_rows, halo_rows)

    def one_device(block):
        inner_adj, halo_adj, own_rows, remote_rows = block
        return jnp.dot(inner_adj, own_rows, preferred_element_type=jnp.float32) + jnp.dot(halo_adj, remote_rows, preferred_element_type=jnp.float32)

    return lax.map(one_device, blocks).reshape(GROUP_SIZE * NODES_DEV, feat_width)


def aggregate_back(a_int, a_halo, grad_rows, send_idx):
    feat_width = grad_rows.shape[-1]
    local_rows = grad_rows.reshape(GROUP_SIZE, NODES_DEV, feat_width)
    blocks = (a_int.reshape(GROUP_SIZE, NODES_DEV, NODES_DEV), a_halo.reshape(GROUP_SIZE, NODES_DEV, NUM_LINKS * HALO_SLOTS), local_rows)

    def one_device(block):
        inner_adj, halo_adj, own_rows = block
        inner_sum = jnp.dot(inner_adj.T, own_rows, preferred_element_type=jnp.float32)
        outward = jnp.dot(halo_adj.T, own_rows, preferred_element_type=jnp.float32).astype(jnp.bfloat16)
        return inner_sum, outward

    inner_sum, outward = lax.map(one_device, blocks)
    outward = outward.reshape(GROUP_SIZE, NUM_LINKS, HALO_SLOTS, feat_width)
    returned = jnp.stack([jnp.roll(outward[:, link], -OFFSETS[link], axis=0) for link in range(NUM_LINKS)], axis=1)
    returned = returned.reshape(GROUP_SIZE, NUM_LINKS * HALO_SLOTS, feat_width)
    send_plan = send_idx.reshape(GROUP_SIZE, NUM_LINKS * HALO_SLOTS)
    total_sum = jax.vmap(lambda sums_dev, plan_dev, rows_dev: sums_dev.at[plan_dev].add(rows_dev.astype(jnp.float32)))(inner_sum, send_plan, returned)
    return total_sum.reshape(GROUP_SIZE * NODES_DEV, feat_width)


def reference(node_feats, a_int, a_halo, send_idx, w_first, w_second, grad_out):
    z_first = aggregate(a_int, a_halo, node_feats, send_idx).astype(jnp.bfloat16)
    hidden = jnp.maximum(jnp.dot(z_first, w_first, preferred_element_type=jnp.float32), 0.0).astype(jnp.bfloat16)
    z_second = aggregate(a_int, a_halo, hidden, send_idx).astype(jnp.bfloat16)
    dw_second = jnp.dot(z_second.T, grad_out, preferred_element_type=jnp.float32)
    dz_second = jnp.dot(grad_out, w_second.T, preferred_element_type=jnp.float32).astype(jnp.bfloat16)
    d_hidden = aggregate_back(a_int, a_halo, dz_second, send_idx)
    grad_pre = jnp.where(hidden > 0, d_hidden, 0.0).astype(jnp.bfloat16)
    dw_first = jnp.dot(z_first.T, grad_pre, preferred_element_type=jnp.float32)
    dz_first = jnp.dot(grad_pre, w_first.T, preferred_element_type=jnp.float32).astype(jnp.bfloat16)
    grad_feats = aggregate_back(a_int, a_halo, dz_first, send_idx)
    return (dw_first, dw_second, grad_feats)
```

```python
import jax
import jax.numpy as jnp
from jax import lax
from jax.sharding import PartitionSpec as P


def link_offsets(num_links):
    return [(link // 2 + 1) * (1 - 2 * (link % 2)) for link in range(num_links)]


def shift_pairs(axis_size, offset):
    return [(source, (source + offset) % axis_size) for source in range(axis_size)]


def contract_rows(left_rows, right_rows):
    return lax.dot_general(left_rows, right_rows, (((0,), (0,)), ((), ())), preferred_element_type=jnp.float32)


def halo_rows(features, send_idx, axis_size):
    sent_rows = jnp.take(features, send_idx, axis=0)
    received = [lax.ppermute(sent_rows[link], "nodes", shift_pairs(axis_size, offset)) for link, offset in enumerate(link_offsets(send_idx.shape[0]))]
    return jnp.concatenate(received, axis=0)


def aggregate(a_int, a_halo, features, send_idx, axis_size):
    remote = halo_rows(features, send_idx, axis_size)
    return jnp.dot(a_int, features, preferred_element_type=jnp.float32) + jnp.dot(a_halo, remote, preferred_element_type=jnp.float32)


def aggregate_back(a_int, a_halo, grad_rows, send_idx, axis_size):
    num_slots = send_idx.shape[1]
    inner_sum = contract_rows(a_int, grad_rows)
    outward = contract_rows(a_halo, grad_rows).astype(jnp.bfloat16)
    received = [lax.ppermute(outward[link * num_slots:(link + 1) * num_slots], "nodes", shift_pairs(axis_size, -offset)) for link, offset in enumerate(link_offsets(send_idx.shape[0]))]
    returned = jnp.concatenate(received, axis=0).astype(jnp.float32)
    return inner_sum.at[send_idx.reshape(-1)].add(returned)


def solution(mesh):
    axis_size = mesh.shape["nodes"]
    row_spec = P(("graph", "nodes"), None)
    replicated = P(None, None)
    part_spec = P("graph", None)

    def device_step(node_feats, a_int, a_halo, send_idx, w_first, w_second, grad_out):
        classes = grad_out.shape[1]
        pulled = aggregate_back(a_int, a_halo, grad_out, send_idx, axis_size)
        pulled_high = pulled.astype(jnp.bfloat16)
        pulled_low = (pulled - pulled_high.astype(jnp.float32)).astype(jnp.bfloat16)
        pulled_pair = jnp.concatenate([pulled_high, pulled_low], axis=1)
        w_pair = jnp.concatenate([w_second, w_second], axis=1)
        z_first = aggregate(a_int, a_halo, node_feats, send_idx, axis_size).astype(jnp.bfloat16)
        hidden = jnp.maximum(jnp.dot(z_first, w_first, preferred_element_type=jnp.float32), 0.0).astype(jnp.bfloat16)
        second_pair = contract_rows(hidden, pulled_pair)
        dw_second = lax.psum(second_pair[:, :classes] + second_pair[:, classes:], "nodes")
        d_hidden = lax.dot_general(pulled_pair, w_pair, (((1,), (1,)), ((), ())), preferred_element_type=jnp.float32)
        grad_pre = jnp.where(hidden > 0, d_hidden, 0.0).astype(jnp.bfloat16)
        dw_first = lax.psum(contract_rows(z_first, grad_pre), "nodes")
        dz_first = lax.dot_general(grad_pre, w_first, (((1,), (1,)), ((), ())), preferred_element_type=jnp.float32).astype(jnp.bfloat16)
        grad_feats = aggregate_back(a_int, a_halo, dz_first, send_idx, axis_size)
        return dw_first, dw_second, grad_feats

    return jax.shard_map(device_step, mesh=mesh, in_specs=(row_spec, row_spec, row_spec, row_spec, replicated, replicated, row_spec), out_specs=(part_spec, part_spec, row_spec), check_vma=False)
```

```python
import functools

import jax
import jax.numpy as jnp
from jax import lax
from jax.experimental import pallas as pl
from jax.experimental.pallas import tpu as pltpu
from jax.sharding import PartitionSpec as P

BF16, F32 = jnp.bfloat16, jnp.float32
MESH = pl.DeviceIdType.MESH
LANES = 128


def link_offsets(num_links):
    return [(link // 2 + 1) * (1 - 2 * (link % 2)) for link in range(num_links)]


def round_up(size, unit):
    return -(-size // unit) * unit


def dot(left, right):
    return jnp.dot(left, right, preferred_element_type=F32)


def pad_lanes(value, width):
    return jnp.concatenate([value, jnp.zeros((value.shape[0], width - value.shape[1]), value.dtype)], axis=1)


def pad_rows(value, height):
    return jnp.concatenate([value, jnp.zeros((height - value.shape[0], value.shape[1]), value.dtype)], axis=0)


def gcn_kernel(axis_size, names, *refs):
    r = dict(zip(names, refs, strict=True))
    feats_hbm, aint_hbm, ahalo_hbm, idx_hbm = r["feats_hbm"], r["aint_hbm"], r["ahalo_hbm"], r["idx_hbm"]
    feats, aint, ahalo, idx, w1, w2, g = (r[k] for k in ("feats", "aint", "ahalo", "idx", "w1", "w2", "g"))
    nodes, feat_in = feats.shape
    hidden, classes = w2.shape
    links, slots = idx.shape
    halo = links * slots
    offsets = link_offsets(links)
    feat_pad = r["featp"].shape[1]
    class_pad = r["gT"].shape[0]
    class_rows = r["precv"].shape[0]
    feat_rows = r["e0T"].shape[0]
    block = 512
    num_blocks = nodes // block
    me = lax.axis_index("nodes")
    chips = axis_size // 2
    core = me % 2
    sign = 1 - 2 * core
    chip = me // 2

    def at_offset(offset):
        return (me + offset + axis_size) % axis_size

    def remote(src, dst, send_sem, recv_sem, target):
        return pltpu.make_async_remote_copy(src_ref=src, dst_ref=dst, send_sem=send_sem, recv_sem=recv_sem, device_id={"nodes": target}, device_id_type=MESH)

    lsem = r["local_sem"]
    small = [(idx_hbm, idx), (feats_hbm, feats), (r["g_hbm"], g), (r["w1_hbm"], w1), (r["w2_hbm"], w2)]
    pairs = small + [(ahalo_hbm.at[:, pl.ds(k * slots, slots)], ahalo.at[:, pl.ds(k * slots, slots)]) for k in range(links)]
    pairs += [(aint_hbm.at[:, pl.ds(j * block, block)], aint.at[:, pl.ds(j * block, block)]) for j in range(num_blocks)]
    copies = [pltpu.make_async_copy(src, dst, lsem.at[i]) for i, (src, dst) in enumerate(pairs)]
    for copy in copies:
        copy.start()
    c_idx, c_feats, c_g, c_w1, c_w2 = copies[:5]
    c_ahalo, c_aint = copies[5:5 + links], copies[5 + links:]

    barrier = pltpu.get_barrier_semaphore()
    peers = [1, -1, 2, -2, 4, -4]
    for offset in peers:
        pl.semaphore_signal(barrier, inc=1, device_id={"nodes": at_offset(offset)}, device_id_type=MESH)

    c_idx.wait()
    sel = r["sel"]
    r["idxp"][...] = jnp.zeros(r["idxp"].shape, F32)
    r["idxp"][0:links, :] = idx[...].astype(F32)
    r["idxT"][...] = r["idxp"][...].T
    step = 64
    for k in range(links):
        def fill(i, carry, k=k):
            col = r["idxT"][pl.ds(pl.multiple_of(i * step, step), step), k:k + 1]
            lane = lax.broadcasted_iota(jnp.int32, (step, nodes), 1).astype(F32)
            row = pl.multiple_of(k * slots + i * step, step)
            sel[pl.ds(row, step), :] = jnp.where(lane == col, 1.0, 0.0).astype(BF16)
            return carry
        lax.fori_loop(0, slots // step, fill, 0)

    c_feats.wait()
    featp = r["featp"]
    for b in range(num_blocks):
        rows = pl.ds(b * block, block)
        featp[rows, :] = pad_lanes(feats[rows, :], feat_pad)
    hsends = []
    for k in (2, 3, 0, 1):
        rows = pl.ds(k * slots, slots)
        r["hsend"][k] = dot(sel[rows, :], featp[...]).astype(BF16)
        if not hsends:
            pl.semaphore_wait(barrier, len(peers))
        copy = remote(r["hsend"].at[k], r["hrecv"].at[rows], r["h_ssem"].at[k], r["h_rsem"].at[k], at_offset(offsets[k]))
        copy.start()
        hsends.append(copy)

    c_g.wait()
    gT, pT = r["gT"], r["pT"]
    for b in range(num_blocks):
        rows = pl.ds(b * block, block)
        gT[:, rows] = pad_lanes(g[rows, :].astype(F32), class_pad).T.astype(BF16)
    psends = []
    for k in (2, 3, 0, 1):
        cols = pl.ds(k * slots, slots)
        c_ahalo[k].wait()
        r["psend"][k] = dot(gT[...], ahalo[:, cols])[0:class_rows].astype(BF16)
        copy = remote(r["psend"].at[k], r["precv"].at[:, cols], r["p_ssem"].at[k], r["p_rsem"].at[k], at_offset(-offsets[k]))
        copy.start()
        psends.append(copy)
    for b in range(num_blocks):
        cols = pl.ds(b * block, block)
        c_aint[b].wait()
        pT[:, cols] = dot(gT[...], aint[:, cols])

    zf, zb, zT, h1T = r["zf"], r["zb"], r["zT"], r["h1T"]
    for b in range(num_blocks):
        rows = pl.ds(b * block, block)
        zf[rows, :] = dot(aint[rows, :], featp[...])
    c_w1.wait()
    c_w2.wait()
    w1p = r["w1p"]
    w1p[...] = pad_rows(w1[...], feat_rows)
    r["w1T"][...] = pad_rows(w1[...].astype(F32), feat_pad).T.astype(BF16)
    w2v = pad_lanes(w2[...], class_pad)
    r["w2p"][...] = jnp.concatenate([w2v, w2v], axis=1)
    for copy in hsends:
        copy.wait_recv()
    for b in range(num_blocks):
        rows = pl.ds(b * block, block)
        z = zf[rows, :] + dot(ahalo[rows, :], r["hrecv"][...])
        zb[rows, :] = z.astype(BF16)
        zT[:, rows] = z.T.astype(BF16)
    for b in range(num_blocks):
        cols = pl.ds(b * block, block)
        h1T[:, cols] = jnp.maximum(dot(r["w1T"][...], zT[:, cols]), 0.0).astype(BF16)

    for copy in psends:
        copy.wait_recv()
    pairT, pair = r["pairT"], r["pair"]
    for b in range(num_blocks):
        cols = pl.ds(b * block, block)
        total = pT[:, cols] + pad_rows(dot(r["precv"][...], sel[:, cols]), class_pad)
        high = total.astype(BF16)
        low = total - high.astype(F32)
        pairT[0:class_pad, cols] = high
        pairT[class_pad:2 * class_pad, cols] = low.astype(BF16)
        pair[cols, 0:class_pad] = total.T.astype(BF16)
        pair[cols, class_pad:2 * class_pad] = low.T.astype(BF16)

    part, full = r["part"], r["full"]
    rows2, rows1 = hidden // axis_size, part.shape[1] - hidden // axis_size
    lane_groups = hidden // LANES
    second = dot(h1T[...], pair[...])
    second = second[:, 0:class_pad] + second[:, class_pad:2 * class_pad]
    for q in range(axis_size):
        part[q, 0:rows2, :] = second[q * rows2:(q + 1) * rows2]
    fT = r["fT"]
    for b in range(num_blocks):
        cols = pl.ds(b * block, block)
        d1T = dot(r["w2p"][...], pairT[:, cols])
        fT[:, cols] = jnp.where(h1T[:, cols].astype(F32) > 0, d1T, 0.0).astype(BF16)
    first = dot(fT[...], zb[...]).T
    for q in range(axis_size):
        row, lane = (q // lane_groups) * rows1, (q % lane_groups) * LANES
        part[q, rows2:rows2 + rows1, :] = first[row:row + rows1, lane:lane + LANES]

    half = core * chips
    other = (1 - core) * chips
    arsem_s, arsem_r = r["ar_ssem"], r["ar_rsem"]
    started = []

    def send(slot, src, dst, target):
        copy = remote(src, dst, arsem_s.at[slot], arsem_r.at[slot], target)
        copy.start()
        started.append(copy)
        return copy

    def chip_at(distance):
        return (chip + distance * sign + 2 * chips) % chips

    def device_at(distance):
        return chip_at(distance) * 2 + core

    sibling = me + sign
    mine, arbuf = r["mine"], r["arbuf"]
    swap = send(0, part.at[pl.ds(other, chips)], r["swap"], sibling)

    e0T, gradT = r["e0T"], r["gradT"]
    for b in range(num_blocks):
        cols = pl.ds(b * block, block)
        e0T[:, cols] = dot(w1p[...], fT[:, cols]).astype(BF16)

    swap.wait_recv()
    mine[...] = part[pl.ds(half, chips)] + r["swap"][...]
    c_a1 = send(1, mine.at[chip_at(-3)], arbuf.at[0], device_at(-1))
    c_a2 = send(2, mine.at[chip_at(4)], arbuf.at[1], device_at(-2))
    c_b = send(3, mine.at[chip_at(3)], arbuf.at[2], device_at(1))
    c_dp = send(4, mine.at[chip_at(-1)], arbuf.at[3], device_at(-1))
    c_dm = send(5, mine.at[chip_at(1)], arbuf.at[4], device_at(1))

    esends = []
    for k in (2, 3, 0, 1):
        cols = pl.ds(k * slots, slots)
        r["esend"][k] = dot(e0T[...], ahalo[:, cols]).astype(BF16)
        copy = remote(r["esend"].at[k], r["erecv"].at[:, cols], r["e_ssem"].at[k], r["e_rsem"].at[k], at_offset(-offsets[k]))
        copy.start()
        esends.append(copy)
    for b in range(num_blocks):
        cols = pl.ds(b * block, block)
        gradT[:, cols] = dot(e0T[...], aint[:, cols])

    c_a1.wait_recv()
    c_a2.wait_recv()
    r["relay"][0] = mine[chip_at(-2)] + arbuf[0] + arbuf[1]
    c_ep = send(6, r["relay"].at[0], arbuf.at[5], device_at(-2))
    c_b.wait_recv()
    r["relay"][1] = mine[chip_at(2)] + arbuf[2]
    c_em = send(7, r["relay"].at[1], arbuf.at[6], device_at(2))

    for copy in esends:
        copy.wait_recv()
    ostage = r["ostage"]
    outs = []
    for b in range(num_blocks):
        cols = pl.ds(b * block, block)
        total = gradT[:, cols] + dot(r["erecv"][...], sel[:, cols])
        ostage[cols, :] = pad_rows(total, feat_pad).T[:, 0:feat_in]
        copy = pltpu.make_async_copy(ostage.at[cols], r["gf_hbm"].at[cols], r["out_sem"].at[b])
        copy.start()
        outs.append(copy)

    for copy in (c_dp, c_dm, c_ep, c_em):
        copy.wait_recv()
    own = half + chip
    full[own] = mine[chip] + arbuf[3] + arbuf[4] + arbuf[5] + arbuf[6]

    def spread(slot, distance, target):
        place = full.at[half + chip_at(distance)]
        return send(slot, place, place, target)

    g_p1 = spread(8, 0, device_at(-1))
    g_m1 = spread(9, 0, device_at(1))
    g_p2 = spread(10, 0, device_at(-2))
    g_m2 = spread(11, 0, device_at(2))
    to_sibling = [spread(15, 0, sibling)]
    g_p2.wait_recv()
    g_p3 = spread(12, 2, device_at(-1))
    g_p4 = spread(13, 2, device_at(-2))
    g_m2.wait_recv()
    g_m3 = spread(14, -2, device_at(1))
    to_sibling.append(spread(16, 2, sibling))
    to_sibling.append(spread(17, -2, sibling))
    g_p1.wait_recv()
    to_sibling.append(spread(18, 1, sibling))
    g_m1.wait_recv()
    to_sibling.append(spread(19, -1, sibling))
    g_p3.wait_recv()
    to_sibling.append(spread(20, 3, sibling))
    g_m3.wait_recv()
    to_sibling.append(spread(21, -3, sibling))
    g_p4.wait_recv()
    to_sibling.append(spread(22, 4, sibling))
    for copy in to_sibling:
        copy.wait_recv()
    for q in range(axis_size):
        r["dw2"][q * rows2:(q + 1) * rows2, :] = full[q, 0:rows2, 0:classes]
        row, lane = (q // lane_groups) * rows1, (q % lane_groups) * LANES
        count = min(rows1, feat_in - row)
        r["dw1"][row:row + count, lane:lane + LANES] = full[q, rows2:rows2 + count, :]
    for copy in started + hsends + psends + esends:
        copy.wait_send()
    for copy in outs:
        copy.wait()


def gcn_backward(axis_size, node_feats, a_int, a_halo, send_idx, w_first, w_second, grad_out):
    nodes, feat_in = node_feats.shape
    hidden, classes = w_second.shape
    links, slots = send_idx.shape
    halo = links * slots
    chips = axis_size // 2
    assert chips == 8 and links == 4
    feat_pad = round_up(feat_in, 2 * LANES)
    feat_rows = round_up(feat_in, 16)
    class_pad = round_up(classes, LANES)
    class_rows = round_up(classes, 16)
    rows2 = hidden // axis_size
    rows1 = round_up(-(-feat_in // (axis_size // (hidden // LANES))), 8)
    chunk = (rows2 + rows1, LANES)
    vmem, dma = pltpu.VMEM, pltpu.SemaphoreType.DMA
    scratch = dict(
        feats=vmem((nodes, feat_in), BF16), aint=vmem((nodes, nodes), BF16), ahalo=vmem((nodes, halo), BF16), idx=vmem((links, slots), jnp.int32),
        w1=vmem((feat_in, hidden), BF16), w2=vmem((hidden, classes), BF16), g=vmem((nodes, classes), BF16),
        featp=vmem((nodes, feat_pad), BF16), idxp=vmem((LANES, slots), F32), idxT=vmem((slots, LANES), F32), sel=vmem((halo, nodes), BF16),
        hsend=vmem((links, slots, feat_pad), BF16), hrecv=vmem((halo, feat_pad), BF16),
        gT=vmem((class_pad, nodes), BF16), pT=vmem((class_pad, nodes), F32), psend=vmem((links, class_rows, slots), BF16), precv=vmem((class_rows, halo), BF16),
        zf=vmem((nodes, feat_pad), F32), zb=vmem((nodes, feat_pad), BF16), zT=vmem((feat_pad, nodes), BF16),
        w1p=vmem((feat_rows, hidden), BF16), w1T=vmem((hidden, feat_pad), BF16), w2p=vmem((hidden, 2 * class_pad), BF16),
        h1T=vmem((hidden, nodes), BF16), fT=vmem((hidden, nodes), BF16), pairT=vmem((2 * class_pad, nodes), BF16), pair=vmem((nodes, 2 * class_pad), BF16),
        e0T=vmem((feat_rows, nodes), BF16), esend=vmem((links, feat_rows, slots), BF16), erecv=vmem((feat_rows, halo), BF16), gradT=vmem((feat_rows, nodes), F32),
        ostage=vmem((nodes, feat_in), F32),
        part=vmem((axis_size,) + chunk, F32), swap=vmem((chips,) + chunk, F32), mine=vmem((chips,) + chunk, F32), arbuf=vmem((7,) + chunk, F32), relay=vmem((2,) + chunk, F32), full=vmem((axis_size,) + chunk, F32),
        local_sem=dma((16,)), out_sem=dma((4,)), h_ssem=dma((links,)), h_rsem=dma((links,)), p_ssem=dma((links,)), p_rsem=dma((links,)), e_ssem=dma((links,)), e_rsem=dma((links,)), ar_ssem=dma((23,)), ar_rsem=dma((23,)))
    names = ["feats_hbm", "aint_hbm", "ahalo_hbm", "idx_hbm", "w1_hbm", "w2_hbm", "g_hbm", "dw1", "dw2", "gf_hbm"] + list(scratch)
    any_spec = pl.BlockSpec(memory_space=pl.ANY)
    vmem_spec = pl.BlockSpec(memory_space=pltpu.VMEM)
    return pl.pallas_call(
        functools.partial(gcn_kernel, axis_size, names),
        out_shape=(jax.ShapeDtypeStruct((feat_in, hidden), F32), jax.ShapeDtypeStruct((hidden, classes), F32), jax.ShapeDtypeStruct((nodes, feat_in), F32)),
        in_specs=[any_spec] * 7,
        out_specs=(vmem_spec, vmem_spec, any_spec),
        scratch_shapes=list(scratch.values()),
        compiler_params=pltpu.CompilerParams(collective_id=0, has_side_effects=True, vmem_limit_bytes=62 * 1024 * 1024),
    )(node_feats, a_int, a_halo, send_idx, w_first, w_second, grad_out)


def solution(mesh):
    axis_size = mesh.shape["nodes"]
    row_spec = P(("graph", "nodes"), None)
    replicated = P(None, None)
    part_spec = P("graph", None)
    step = functools.partial(gcn_backward, axis_size)
    return jax.shard_map(step, mesh=mesh, in_specs=(row_spec, row_spec, row_spec, row_spec, replicated, replicated, row_spec), out_specs=(part_spec, part_spec, row_spec), check_vma=False)
```

```python
import functools

import jax
import jax.numpy as jnp
from jax import lax
from jax.experimental import pallas as pl
from jax.experimental.pallas import tpu as pltpu
from jax.sharding import PartitionSpec as P

BF16, F32 = jnp.bfloat16, jnp.float32
MESH = pl.DeviceIdType.MESH
LANES = 128
VMEM_MIB = 56


def link_offsets(num_links):
    return [(link // 2 + 1) * (1 - 2 * (link % 2)) for link in range(num_links)]


def round_up(size, unit):
    return -(-size // unit) * unit


def dot(left, right):
    return jnp.dot(left, right, preferred_element_type=F32)


def dot_lanes(left, right):
    return lax.dot_general(left, right, (((1,), (1,)), ((), ())), preferred_element_type=F32)


def pad_lanes(value, width):
    return jnp.concatenate([value, jnp.zeros((value.shape[0], width - value.shape[1]), value.dtype)], axis=1)


def pad_rows(value, height):
    return jnp.concatenate([value, jnp.zeros((height - value.shape[0], value.shape[1]), value.dtype)], axis=0)


def gcn_kernel(axis_size, names, *refs):
    r = dict(zip(names, refs, strict=True))
    featsT, aint, ahalo, idx, w1, w2T, gT = (r[k] for k in ("featsT", "aint", "ahalo", "idx", "w1", "w2T", "gT"))
    feat_in, nodes = featsT.shape
    classes, hidden = w2T.shape
    links, slots = idx.shape
    halo = links * slots
    offsets = link_offsets(links)
    feat_pad = r["featp"].shape[0]
    class_pad = r["pT"].shape[0]
    class_rows = r["precv"].shape[0]
    feat_rows = r["e0T"].shape[0]
    block = 512
    num_blocks = nodes // block
    me = lax.axis_index("nodes")
    chips = axis_size // 2
    core = me % 2
    sign = 1 - 2 * core
    chip = me // 2
    order = (2, 3, 0, 1)

    def at_offset(offset):
        return (me + offset + axis_size) % axis_size

    def remote(src, dst, send_sem, recv_sem, target):
        return pltpu.make_async_remote_copy(src_ref=src, dst_ref=dst, send_sem=send_sem, recv_sem=recv_sem, device_id={"nodes": target}, device_id_type=MESH)

    lsem = r["local_sem"]
    pairs = [(r["idx_hbm"], idx), (r["featsT_hbm"], featsT), (r["gT_hbm"], gT)]
    row_blocks = [pl.ds(b * block, block) for b in range(num_blocks)]
    pairs += [(r["ahalo_hbm"].at[rows], ahalo.at[rows]) for rows in row_blocks]
    pairs += [(r["w1_hbm"], w1), (r["w2T_hbm"], w2T)]
    pairs += [(r["aint_hbm"].at[rows], aint.at[rows]) for rows in row_blocks]
    copies = [pltpu.make_async_copy(src, dst, lsem.at[i]) for i, (src, dst) in enumerate(pairs)]
    for copy in copies:
        copy.start()
    c_idx, c_feats, c_g = copies[:3]
    c_ahalo, (c_w1, c_w2), c_aint = copies[3:3 + num_blocks], copies[3 + num_blocks:5 + num_blocks], copies[5 + num_blocks:]

    barrier = pltpu.get_barrier_semaphore()
    peers = [1, -1, 2, -2, 4, -4]
    for offset in peers:
        pl.semaphore_signal(barrier, inc=1, device_id={"nodes": at_offset(offset)}, device_id_type=MESH)
    for k in range(links):
        r["hrecv"][k, feat_rows:feat_pad, :] = jnp.zeros((feat_pad - feat_rows, slots), BF16)

    c_idx.wait()
    pick = r["pick"]
    sub = 16
    hsends = []
    for k in order:
        index = idx[k:k + 1, :]
        low = jnp.broadcast_to(index % sub, (sub, slots))
        high = jnp.broadcast_to((index // sub).astype(F32), (sub, slots)).astype(BF16)
        ones = jnp.where(lax.broadcasted_iota(jnp.int32, (sub, slots), 0) == low, 1.0, 0.0).astype(BF16)
        zeros = jnp.zeros((sub, slots), BF16)
        for m in range(nodes // sub):
            pick[k % 2, m * sub:(m + 1) * sub, :] = jnp.where(high == jnp.array(m, BF16), ones, zeros)
        if not hsends:
            c_feats.wait()
        r["hsend"][k] = pad_rows(dot(featsT[...], pick[k % 2]), feat_rows).astype(BF16)
        if not hsends:
            pl.semaphore_wait(barrier, len(peers))
        copy = remote(r["hsend"].at[k], r["hrecv"].at[k, pl.ds(0, feat_rows)], r["h_ssem"].at[k], r["h_rsem"].at[k], at_offset(offsets[k]))
        copy.start()
        hsends.append(copy)

    c_g.wait()
    for copy in c_ahalo:
        copy.wait()
    psends = []
    for k in order:
        cols = pl.ds(k * slots, slots)
        r["psend"][k] = pad_rows(dot(gT[...], ahalo[:, cols]), class_rows).astype(BF16)
        copy = remote(r["psend"].at[k], r["precv"].at[:, cols], r["p_ssem"].at[k], r["p_rsem"].at[k], at_offset(-offsets[k]))
        copy.start()
        psends.append(copy)

    sel = r["sel"]
    r["idxp"][...] = jnp.zeros(r["idxp"].shape, F32)
    r["idxp"][0:links, :] = idx[...].astype(F32)
    r["idxT"][...] = r["idxp"][...].T
    step = 64
    for k in range(links):
        def fill(i, carry, k=k):
            col = r["idxT"][pl.ds(pl.multiple_of(i * step, step), step), k:k + 1]
            tile = jnp.floor(col * (1.0 / LANES))
            lane = lax.broadcasted_iota(jnp.int32, (step, LANES), 1).astype(F32)
            ones = jnp.where(lane == col - tile * LANES, 1.0, 0.0).astype(BF16)
            tile = jnp.broadcast_to(tile, (step, LANES)).astype(BF16)
            row = pl.multiple_of(k * slots + i * step, step)
            for t in range(nodes // LANES):
                sel[pl.ds(row, step), t * LANES:(t + 1) * LANES] = jnp.where(tile == jnp.array(t, BF16), ones, jnp.zeros((step, LANES), BF16))
            return carry
        lax.fori_loop(0, slots // step, fill, 0)

    featp, pT = r["featp"], r["pT"]
    featp[...] = pad_rows(featsT[...], feat_pad)
    zf, zb, zT, h1T = r["zf"], r["zb"], r["zT"], r["h1T"]
    for b in range(num_blocks):
        rows = pl.ds(b * block, block)
        c_aint[b].wait()
        zf[rows, :] = dot_lanes(aint[rows, :], featp[...])
    c_w1.wait()
    c_w2.wait()
    w1p = r["w1p"]
    w1p[...] = pad_rows(w1[...], feat_rows)
    r["w1T"][...] = pad_rows(w1[...].astype(F32), feat_pad).T.astype(BF16)
    w2v = pad_rows(w2T[...].astype(F32), class_pad).T.astype(BF16)
    r["w2p"][...] = jnp.concatenate([w2v, w2v], axis=1)
    for b in range(num_blocks):
        cols = pl.ds(b * block, block)
        pT[:, cols] = pad_rows(dot(gT[...], aint[:, cols]), class_pad)

    for i, k in enumerate(order):
        cols = pl.ds(k * slots, slots)
        hsends[i].wait_recv()
        for b in range(num_blocks):
            rows = pl.ds(b * block, block)
            z = zf[rows, :] + dot_lanes(ahalo[rows, cols], r["hrecv"][k])
            if i < links - 1:
                zf[rows, :] = z
            else:
                zb[rows, :] = z.astype(BF16)
                zT[:, rows] = z.T.astype(BF16)
    for b in range(num_blocks):
        cols = pl.ds(b * block, block)
        h1T[:, cols] = jnp.maximum(dot(r["w1T"][...], zT[:, cols]), 0.0).astype(BF16)

    for copy in psends:
        copy.wait_recv()
    pairT, pair = r["pairT"], r["pair"]
    for b in range(num_blocks):
        cols = pl.ds(b * block, block)
        total = pT[:, cols] + pad_rows(dot(r["precv"][...], sel[:, cols]), class_pad)
        high = total.astype(BF16)
        low = total - high.astype(F32)
        pairT[0:class_pad, cols] = high
        pairT[class_pad:2 * class_pad, cols] = low.astype(BF16)
        pair[cols, 0:class_pad] = total.T.astype(BF16)
        pair[cols, class_pad:2 * class_pad] = low.T.astype(BF16)

    fT = r["fT"]
    for b in range(num_blocks):
        cols = pl.ds(b * block, block)
        d1T = dot(r["w2p"][...], pairT[:, cols])
        fT[:, cols] = jnp.where(h1T[:, cols].astype(F32) > 0, d1T, 0.0).astype(BF16)
    part, full = r["part"], r["full"]
    pieces, rows_piece = part.shape[0], part.shape[2]
    lane_groups = hidden // LANES
    second = dot(h1T[...], pair[...])
    second = (second[:, 0:class_pad] + second[:, class_pad:2 * class_pad]).T
    first = dot(fT[...], zb[...]).T

    def places():
        for q in range(axis_size):
            for p in range(pieces):
                row = ((q // lane_groups) * pieces + p) * rows_piece
                yield p, q, row, pl.ds((q % lane_groups) * LANES, LANES)

    for p, q, row, lane in places():
        lanes = slice(lane.start, lane.start + LANES)
        if row < feat_in:
            part[p, q] = first[row:row + rows_piece, lanes]
        else:
            part[p, q] = second[row - feat_in:row - feat_in + rows_piece, lanes]

    half = core * chips
    other = (1 - core) * chips
    arsem_s, arsem_r = r["ar_ssem"], r["ar_rsem"]
    started = []

    def send(piece, slot, src, dst, target):
        copy = remote(src, dst, arsem_s.at[piece, slot], arsem_r.at[piece, slot], target)
        copy.start()
        started.append(copy)
        return copy

    def chip_at(distance):
        return (chip + distance * sign + 2 * chips) % chips

    def device_at(distance):
        return chip_at(distance) * 2 + core

    sibling = me + sign
    mine, arbuf, relay = r["mine"], r["arbuf"], r["relay"]
    swap = [send(p, 0, part.at[p, pl.ds(other, chips)], r["swap"].at[p], sibling) for p in range(pieces)]

    e0T, gradT = r["e0T"], r["gradT"]
    for b in range(num_blocks):
        cols = pl.ds(b * block, block)
        e0T[:, cols] = dot(w1p[...], fT[:, cols]).astype(BF16)

    first_step = []
    for p in range(pieces):
        swap[p].wait_recv()
        mine[p] = part[p, pl.ds(half, chips)] + r["swap"][p]
        first_step.append([
            send(p, 1, mine.at[p, chip_at(-3)], arbuf.at[p, 0], device_at(-1)),
            send(p, 2, mine.at[p, chip_at(4)], arbuf.at[p, 1], device_at(-2)),
            send(p, 3, mine.at[p, chip_at(3)], arbuf.at[p, 2], device_at(1)),
            send(p, 4, mine.at[p, chip_at(-1)], arbuf.at[p, 3], device_at(-1)),
            send(p, 5, mine.at[p, chip_at(1)], arbuf.at[p, 4], device_at(1))])

    esends = []
    for k in order:
        cols = pl.ds(k * slots, slots)
        r["esend"][k] = dot(e0T[...], ahalo[:, cols]).astype(BF16)
        copy = remote(r["esend"].at[k], r["erecv"].at[:, cols], r["e_ssem"].at[k], r["e_rsem"].at[k], at_offset(-offsets[k]))
        copy.start()
        esends.append(copy)
    for b in range(num_blocks):
        cols = pl.ds(b * block, block)
        gradT[:, cols] = dot(e0T[...], aint[:, cols])

    second_step = []
    for p in range(pieces):
        c_a1, c_a2, c_b = first_step[p][:3]
        c_a1.wait_recv()
        c_a2.wait_recv()
        relay[p, 0] = mine[p, chip_at(-2)] + arbuf[p, 0] + arbuf[p, 1]
        c_ep = send(p, 6, relay.at[p, 0], arbuf.at[p, 5], device_at(-2))
        c_b.wait_recv()
        relay[p, 1] = mine[p, chip_at(2)] + arbuf[p, 2]
        c_em = send(p, 7, relay.at[p, 1], arbuf.at[p, 6], device_at(2))
        second_step.append([c_ep, c_em])

    for copy in esends:
        copy.wait_recv()
    for b in range(num_blocks):
        cols = pl.ds(b * block, block)
        total = gradT[:, cols] + dot(r["erecv"][...], sel[:, cols])
        r["gfT"][:, cols] = total[0:feat_in]

    spreads = []

    def spread(piece, slot, distance, target):
        place = full.at[piece, half + chip_at(distance)]
        return send(piece, slot, place, place, target)

    for p in range(pieces):
        for copy in first_step[p][3:] + second_step[p]:
            copy.wait_recv()
        full[p, half + chip] = mine[p, chip] + arbuf[p, 3] + arbuf[p, 4] + arbuf[p, 5] + arbuf[p, 6]
        spreads.append([spread(p, 10, 0, device_at(-2)), spread(p, 11, 0, device_at(2)), spread(p, 8, 0, device_at(-1)), spread(p, 9, 0, device_at(1)), spread(p, 15, 0, sibling)])
    lasts = []
    for p in range(pieces):
        g_p2, g_m2, g_p1, g_m1, to_sibling = spreads[p]
        g_p2.wait_recv()
        g_p4 = spread(p, 13, 2, device_at(-2))
        g_p3 = spread(p, 12, 2, device_at(-1))
        g_m2.wait_recv()
        g_m3 = spread(p, 14, -2, device_at(1))
        back = [to_sibling, spread(p, 16, 2, sibling), spread(p, 17, -2, sibling)]
        g_p1.wait_recv()
        back.append(spread(p, 18, 1, sibling))
        g_m1.wait_recv()
        back.append(spread(p, 19, -1, sibling))
        lasts.append([g_p3, g_m3, g_p4, back])
    for p in range(pieces):
        g_p3, g_m3, g_p4, back = lasts[p]
        g_p3.wait_recv()
        back.append(spread(p, 20, 3, sibling))
        g_m3.wait_recv()
        back.append(spread(p, 21, -3, sibling))
        g_p4.wait_recv()
        back.append(spread(p, 22, 4, sibling))
    for p in range(pieces):
        for copy in lasts[p][3]:
            copy.wait_recv()
    for p, q, row, lane in places():
        if row < feat_in:
            r["dw1"][row:row + rows_piece, lane] = full[p, q]
        else:
            row = row - feat_in
            count = min(rows_piece, classes - row)
            r["dw2T"][row:row + count, lane] = full[p, q, 0:count, :]
    for copy in started + hsends + psends + esends:
        copy.wait_send()


def gcn_backward(axis_size, node_feats, a_int, a_halo, send_idx, w_first, w_second, grad_out):
    nodes, feat_in = node_feats.shape
    hidden, classes = w_second.shape
    links, slots = send_idx.shape
    halo = links * slots
    chips = axis_size // 2
    pieces = 2
    feat_pad = round_up(feat_in, 2 * LANES)
    feat_rows = round_up(feat_in, 16)
    class_pad = round_up(classes, LANES)
    class_rows = round_up(classes, 16)
    row_groups = axis_size // (hidden // LANES)
    rows_piece = round_up(-(-(feat_in + classes) // (row_groups * pieces)), 8)
    assert chips == 8 and links == 4 and feat_in % rows_piece == 0 and classes <= row_groups * pieces * rows_piece - feat_in <= class_pad
    chunk = (rows_piece, LANES)
    vmem, dma = pltpu.VMEM, pltpu.SemaphoreType.DMA
    scratch = dict(
        featsT=vmem((feat_in, nodes), BF16), aint=vmem((nodes, nodes), BF16), ahalo=vmem((nodes, halo), BF16), idx=vmem((links, slots), jnp.int32),
        w1=vmem((feat_in, hidden), BF16), w2T=vmem((classes, hidden), BF16), gT=vmem((classes, nodes), BF16),
        featp=vmem((feat_pad, nodes), BF16), idxp=vmem((LANES, slots), F32), idxT=vmem((slots, LANES), F32), pick=vmem((2, nodes, slots), BF16), sel=vmem((halo, nodes), BF16),
        hsend=vmem((links, feat_rows, slots), BF16), hrecv=vmem((links, feat_pad, slots), BF16),
        pT=vmem((class_pad, nodes), F32), psend=vmem((links, class_rows, slots), BF16), precv=vmem((class_rows, halo), BF16),
        zf=vmem((nodes, feat_pad), F32), zb=vmem((nodes, feat_pad), BF16), zT=vmem((feat_pad, nodes), BF16),
        w1p=vmem((feat_rows, hidden), BF16), w1T=vmem((hidden, feat_pad), BF16), w2p=vmem((hidden, 2 * class_pad), BF16),
        h1T=vmem((hidden, nodes), BF16), fT=vmem((hidden, nodes), BF16), pairT=vmem((2 * class_pad, nodes), BF16), pair=vmem((nodes, 2 * class_pad), BF16),
        e0T=vmem((feat_rows, nodes), BF16), esend=vmem((links, feat_rows, slots), BF16), erecv=vmem((feat_rows, halo), BF16), gradT=vmem((feat_rows, nodes), F32),
        part=vmem((pieces, axis_size) + chunk, F32), swap=vmem((pieces, chips) + chunk, F32), mine=vmem((pieces, chips) + chunk, F32), arbuf=vmem((pieces, 7) + chunk, F32), relay=vmem((pieces, 2) + chunk, F32), full=vmem((pieces, axis_size) + chunk, F32),
        local_sem=dma((16,)), h_ssem=dma((links,)), h_rsem=dma((links,)), p_ssem=dma((links,)), p_rsem=dma((links,)), e_ssem=dma((links,)), e_rsem=dma((links,)), ar_ssem=dma((pieces, 23)), ar_rsem=dma((pieces, 23)))
    names = ["featsT_hbm", "aint_hbm", "ahalo_hbm", "idx_hbm", "w1_hbm", "w2T_hbm", "gT_hbm", "dw1", "dw2T", "gfT"] + list(scratch)
    any_spec = pl.BlockSpec(memory_space=pltpu.HBM)
    vmem_spec = pl.BlockSpec(memory_space=pltpu.VMEM)
    dw_first, dw_second, grad_feats = pl.pallas_call(
        functools.partial(gcn_kernel, axis_size, names),
        out_shape=(jax.ShapeDtypeStruct((feat_in, hidden), F32), jax.ShapeDtypeStruct((classes, hidden), F32), jax.ShapeDtypeStruct((feat_in, nodes), F32)),
        in_specs=[any_spec] * 7,
        out_specs=(vmem_spec, vmem_spec, vmem_spec),
        scratch_shapes=list(scratch.values()),
        compiler_params=pltpu.CompilerParams(collective_id=0, has_side_effects=True, vmem_limit_bytes=VMEM_MIB * 1024 * 1024),
    )(node_feats.T, a_int, a_halo, send_idx, w_first, w_second.T, grad_out.T)
    return dw_first, dw_second.T, grad_feats.T


def solution(mesh):
    axis_size = mesh.shape["nodes"]
    row_spec = P(("graph", "nodes"), None)
    replicated = P(None, None)
    part_spec = P("graph", None)
    step = functools.partial(gcn_backward, axis_size)
    return jax.shard_map(step, mesh=mesh, in_specs=(row_spec, row_spec, row_spec, row_spec, replicated, replicated, row_spec), out_specs=(part_spec, part_spec, row_spec), check_vma=False)
```

```python
import functools

import jax
import jax.numpy as jnp
from jax import lax
from jax.experimental import pallas as pl
from jax.experimental.pallas import tpu as pltpu
from jax.sharding import PartitionSpec as P

BF16, F32 = jnp.bfloat16, jnp.float32
MESH = pl.DeviceIdType.MESH
LANES = 128
VMEM_MIB = 50


def link_offsets(num_links):
    return [(link // 2 + 1) * (1 - 2 * (link % 2)) for link in range(num_links)]


def round_up(size, unit):
    return -(-size // unit) * unit


def dot(left, right):
    return jnp.dot(left, right, preferred_element_type=F32)


def dot_lanes(left, right):
    return lax.dot_general(left, right, (((1,), (1,)), ((), ())), preferred_element_type=F32)


def pad_lanes(value, width):
    return jnp.concatenate([value, jnp.zeros((value.shape[0], width - value.shape[1]), value.dtype)], axis=1)


def pad_rows(value, height):
    return jnp.concatenate([value, jnp.zeros((height - value.shape[0], value.shape[1]), value.dtype)], axis=0)


def gcn_kernel(axis_size, names, *refs):
    r = dict(zip(names, refs, strict=True))
    featsT, aint, ahalo, idx, w1, w2T, gT = (r[k] for k in ("featsT", "aint", "ahalo", "idx", "w1", "w2T", "gT"))
    feat_in, nodes = featsT.shape
    classes, hidden = w2T.shape
    links, slots = idx.shape
    halo = links * slots
    offsets = link_offsets(links)
    feat_pad = r["featp"].shape[0]
    class_pad = r["pT"].shape[0]
    class_rows = r["precv"].shape[0]
    feat_rows = r["e0T"].shape[0]
    block = 512
    num_blocks = nodes // block
    me = lax.axis_index("nodes")
    chips = axis_size // 2
    core = me % 2
    sign = 1 - 2 * core
    chip = me // 2
    order = (2, 3, 0, 1)

    def at_offset(offset):
        return (me + offset + axis_size) % axis_size

    def remote(src, dst, send_sem, recv_sem, target):
        return pltpu.make_async_remote_copy(src_ref=src, dst_ref=dst, send_sem=send_sem, recv_sem=recv_sem, device_id={"nodes": target}, device_id_type=MESH)

    lsem = r["local_sem"]
    pairs = [(r["idx_hbm"], idx), (r["featsT_hbm"], featsT), (r["gT_hbm"], gT)]
    row_blocks = [pl.ds(b * block, block) for b in range(num_blocks)]
    pairs += [(r["ahalo_hbm"].at[rows], ahalo.at[rows]) for rows in row_blocks]
    pairs += [(r["w1_hbm"], w1), (r["w2T_hbm"], w2T)]
    pairs += [(r["aint_hbm"].at[rows], aint.at[rows]) for rows in row_blocks]
    copies = [pltpu.make_async_copy(src, dst, lsem.at[i]) for i, (src, dst) in enumerate(pairs)]
    for copy in copies[:3]:
        copy.start()
    c_idx, c_feats, c_g = copies[:3]
    c_ahalo, (c_w1, c_w2), c_aint = copies[3:3 + num_blocks], copies[3 + num_blocks:5 + num_blocks], copies[5 + num_blocks:]

    barrier = pltpu.get_barrier_semaphore()
    peers = [1, -1, 2, -2, 4, -4]
    for offset in peers:
        pl.semaphore_signal(barrier, inc=1, device_id={"nodes": at_offset(offset)}, device_id_type=MESH)
    for k in range(links):
        r["hrecv"][k, feat_rows:feat_pad, :] = jnp.zeros((feat_pad - feat_rows, slots), BF16)

    c_idx.wait()
    pick = r["pick"]
    sub = 16
    hsends = []
    for k in order:
        index = idx[k:k + 1, :]
        low = jnp.broadcast_to(index % sub, (sub, slots))
        high = jnp.broadcast_to((index // sub).astype(F32), (sub, slots)).astype(BF16)
        ones = jnp.where(lax.broadcasted_iota(jnp.int32, (sub, slots), 0) == low, 1.0, 0.0).astype(BF16)
        zeros = jnp.zeros((sub, slots), BF16)
        for m in range(nodes // sub):
            pick[k % 2, m * sub:(m + 1) * sub, :] = jnp.where(high == jnp.array(m, BF16), ones, zeros)
        if not hsends:
            c_feats.wait()
            for copy in copies[3:]:
                copy.start()
        r["hsend"][k] = pad_rows(dot(featsT[...], pick[k % 2]), feat_rows).astype(BF16)
        if not hsends:
            pl.semaphore_wait(barrier, len(peers))
        copy = remote(r["hsend"].at[k], r["hrecv"].at[k, pl.ds(0, feat_rows)], r["h_ssem"].at[k], r["h_rsem"].at[k], at_offset(offsets[k]))
        copy.start()
        hsends.append(copy)

    c_g.wait()
    for copy in c_ahalo:
        copy.wait()
    psends = []
    for k in order:
        cols = pl.ds(k * slots, slots)
        r["psend"][k] = pad_rows(dot(gT[...], ahalo[:, cols]), class_rows).astype(BF16)
        copy = remote(r["psend"].at[k], r["precv"].at[:, cols], r["p_ssem"].at[k], r["p_rsem"].at[k], at_offset(-offsets[k]))
        copy.start()
        psends.append(copy)

    sel = r["sel"]
    r["idxp"][...] = jnp.zeros(r["idxp"].shape, F32)
    r["idxp"][0:links, :] = idx[...].astype(F32)
    r["idxT"][...] = r["idxp"][...].T
    step = 64
    for k in range(links):
        def fill(i, carry, k=k):
            col = r["idxT"][pl.ds(pl.multiple_of(i * step, step), step), k:k + 1]
            tile = jnp.floor(col * (1.0 / LANES))
            lane = lax.broadcasted_iota(jnp.int32, (step, LANES), 1).astype(F32)
            ones = jnp.where(lane == col - tile * LANES, 1.0, 0.0).astype(BF16)
            tile = jnp.broadcast_to(tile, (step, LANES)).astype(BF16)
            row = pl.multiple_of(k * slots + i * step, step)
            for t in range(nodes // LANES):
                sel[pl.ds(row, step), t * LANES:(t + 1) * LANES] = jnp.where(tile == jnp.array(t, BF16), ones, jnp.zeros((step, LANES), BF16))
            return carry
        lax.fori_loop(0, slots // step, fill, 0)

    featp, pT = r["featp"], r["pT"]
    featp[...] = pad_rows(featsT[...], feat_pad)
    zf, zb, zT, h1T = r["zf"], r["zb"], r["zT"], r["h1T"]
    for b in range(num_blocks):
        rows = pl.ds(b * block, block)
        c_aint[b].wait()
        zf[rows, :] = dot_lanes(aint[rows, :], featp[...])
    c_w1.wait()
    c_w2.wait()
    w1p = r["w1p"]
    w1p[...] = pad_rows(w1[...], feat_rows)
    r["w1T"][...] = pad_rows(w1[...].astype(F32), feat_pad).T.astype(BF16)
    w2v = pad_rows(w2T[...].astype(F32), class_pad).T.astype(BF16)
    r["w2p"][...] = jnp.concatenate([w2v, w2v], axis=1)
    for b in range(num_blocks):
        cols = pl.ds(b * block, block)
        pT[:, cols] = pad_rows(dot(gT[...], aint[:, cols]), class_pad)

    for i, k in enumerate(order):
        cols = pl.ds(k * slots, slots)
        hsends[i].wait_recv()
        for b in range(num_blocks):
            rows = pl.ds(b * block, block)
            z = zf[rows, :] + dot_lanes(ahalo[rows, cols], r["hrecv"][k])
            if i < links - 1:
                zf[rows, :] = z
            else:
                zb[rows, :] = z.astype(BF16)
                zT[:, rows] = z.T.astype(BF16)
    for b in range(num_blocks):
        cols = pl.ds(b * block, block)
        h1T[:, cols] = jnp.maximum(dot(r["w1T"][...], zT[:, cols]), 0.0).astype(BF16)

    pairT, pair = r["pairT"], r["pair"]
    for i, k in enumerate(order):
        slot = pl.ds(k * slots, slots)
        psends[i].wait_recv()
        for b in range(num_blocks):
            cols = pl.ds(b * block, block)
            total = pT[:, cols] + pad_rows(dot(r["precv"][:, slot], sel[slot, cols]), class_pad)
            if i < links - 1:
                pT[:, cols] = total
            else:
                high = total.astype(BF16)
                low = total - high.astype(F32)
                pairT[0:class_pad, cols] = high
                pairT[class_pad:2 * class_pad, cols] = low.astype(BF16)
                pair[cols, 0:class_pad] = total.T.astype(BF16)
                pair[cols, class_pad:2 * class_pad] = low.T.astype(BF16)

    part, full = r["part"], r["full"]
    pieces = piece_rows(feat_in, classes, hidden, axis_size)
    places = tile_places(feat_in, classes, hidden, axis_size)
    half = core * chips
    other = (1 - core) * chips
    arsem_s, arsem_r = r["ar_ssem"], r["ar_rsem"]
    started = []

    def send(piece, slot, src, dst, target):
        copy = remote(src, dst, arsem_s.at[piece, slot], arsem_r.at[piece, slot], target)
        copy.start()
        started.append(copy)
        return copy

    def chip_at(distance):
        return (chip + distance * sign + 2 * chips) % chips

    def device_at(distance):
        return chip_at(distance) * 2 + core

    def rows_of(p):
        return pl.ds(pieces[p][0], pieces[p][1])

    sibling = me + sign
    mine, arbuf, relay = r["mine"], r["arbuf"], r["relay"]
    numbers = range(len(pieces))
    swap, first_step, second_step = {}, {}, {}

    def write_tiles(which, value):
        for q, row, owner, tile_row, lane in places:
            if owner == which:
                part[q, row:row + 8, :] = value[tile_row:tile_row + 8, lane:lane + LANES]

    def start_swap(p):
        swap[p] = send(p, 0, part.at[pl.ds(other, chips), rows_of(p)], r["swap"].at[:, rows_of(p)], sibling)

    def start_first(p):
        rows = rows_of(p)
        swap[p].wait_recv()
        mine[:, rows, :] = part[pl.ds(half, chips), rows, :] + r["swap"][:, rows, :]
        first_step[p] = [
            send(p, 2, mine.at[chip_at(4), rows], arbuf.at[1, rows], device_at(-2)),
            send(p, 1, mine.at[chip_at(-3), rows], arbuf.at[0, rows], device_at(-1)),
            send(p, 3, mine.at[chip_at(3), rows], arbuf.at[2, rows], device_at(1)),
            send(p, 4, mine.at[chip_at(-1), rows], arbuf.at[3, rows], device_at(-1)),
            send(p, 5, mine.at[chip_at(1), rows], arbuf.at[4, rows], device_at(1))]

    def start_second(p):
        rows = rows_of(p)
        c_a2, c_a1, c_b = first_step[p][:3]
        c_b.wait_recv()
        relay[1, rows, :] = mine[chip_at(2), rows, :] + arbuf[2, rows, :]
        c_em = send(p, 7, relay.at[1, rows], arbuf.at[6, rows], device_at(2))
        c_a1.wait_recv()
        c_a2.wait_recv()
        relay[0, rows, :] = mine[chip_at(-2), rows, :] + arbuf[0, rows, :] + arbuf[1, rows, :]
        c_ep = send(p, 6, relay.at[0, rows], arbuf.at[5, rows], device_at(-2))
        second_step[p] = [c_em, c_ep]

    second = dot(h1T[...], pair[...])
    second = (second[:, 0:class_pad] + second[:, class_pad:2 * class_pad]).T
    write_tiles(1, second)
    start_swap(0)
    fT = r["fT"]
    for b in range(num_blocks):
        cols = pl.ds(b * block, block)
        d1T = dot(r["w2p"][...], pairT[:, cols])
        fT[:, cols] = jnp.where(h1T[:, cols].astype(F32) > 0, d1T, 0.0).astype(BF16)
    start_first(0)
    first = dot(fT[...], zb[...]).T
    write_tiles(0, first)
    for p in numbers[1:]:
        start_swap(p)

    e0T, gradT = r["e0T"], r["gradT"]
    for b in range(num_blocks):
        cols = pl.ds(b * block, block)
        e0T[:, cols] = dot(w1p[...], fT[:, cols]).astype(BF16)

    esends = []
    for i, k in enumerate(order):
        cols = pl.ds(k * slots, slots)
        r["esend"][k] = dot(e0T[...], ahalo[:, cols]).astype(BF16)
        if i == 0:
            for p in numbers[1:]:
                start_first(p)
        copy = remote(r["esend"].at[k], r["erecv"].at[:, cols], r["e_ssem"].at[k], r["e_rsem"].at[k], at_offset(-offsets[k]))
        copy.start()
        esends.append(copy)
    start_second(0)
    for b in range(num_blocks):
        cols = pl.ds(b * block, block)
        gradT[:, cols] = dot(e0T[...], aint[:, cols])
    for p in numbers[1:]:
        start_second(p)

    spreads = {}

    def spread(piece, slot, distance, target):
        place = full.at[half + chip_at(distance), rows_of(piece)]
        return send(piece, slot, place, place, target)

    def start_spread(p):
        rows = rows_of(p)
        for copy in first_step[p][3:] + second_step[p]:
            copy.wait_recv()
        full[half + chip, rows, :] = mine[chip, rows, :] + arbuf[3, rows, :] + arbuf[4, rows, :] + arbuf[5, rows, :] + arbuf[6, rows, :]
        spreads[p] = [spread(p, 10, 0, device_at(-2)), spread(p, 11, 0, device_at(2)), spread(p, 8, 0, device_at(-1)), spread(p, 9, 0, device_at(1)), spread(p, 15, 0, sibling)]

    start_spread(0)

    for copy in esends:
        copy.wait_recv()
    for b in range(num_blocks):
        cols = pl.ds(b * block, block)
        total = gradT[:, cols] + dot(r["erecv"][...], sel[:, cols])
        r["gfT"][:, cols] = total[0:feat_in]

    for p in numbers[1:]:
        start_spread(p)
    lasts = []
    for p in numbers:
        g_p2, g_m2, g_p1, g_m1, to_sibling = spreads[p]
        g_p2.wait_recv()
        g_p4 = spread(p, 13, 2, device_at(-2))
        g_p3 = spread(p, 12, 2, device_at(-1))
        g_m2.wait_recv()
        g_m3 = spread(p, 14, -2, device_at(1))
        back = [to_sibling, spread(p, 16, 2, sibling), spread(p, 17, -2, sibling)]
        g_p1.wait_recv()
        back.append(spread(p, 18, 1, sibling))
        g_m1.wait_recv()
        back.append(spread(p, 19, -1, sibling))
        lasts.append([g_p3, g_m3, g_p4, back])
    for p in numbers:
        g_p3, g_m3, g_p4, back = lasts[p]
        g_p3.wait_recv()
        back.append(spread(p, 20, 3, sibling))
        g_m3.wait_recv()
        back.append(spread(p, 21, -3, sibling))
        g_p4.wait_recv()
        back.append(spread(p, 22, 4, sibling))
    for p in numbers:
        for copy in lasts[p][3]:
            copy.wait_recv()
    for q, row, owner, tile_row, lane in places:
        if owner == 0:
            r["dw1"][tile_row:tile_row + 8, lane:lane + LANES] = full[q, row:row + 8, :]
        elif owner == 1:
            count = min(8, classes - tile_row)
            r["dw2T"][tile_row:tile_row + count, lane:lane + LANES] = full[q, row:row + count, :]
    for copy in started + hsends + psends + esends:
        copy.wait_send()


def tile_counts(feat_in, classes, hidden, axis_size):
    lane_groups = hidden // LANES
    first, second = -(-feat_in // 8) * lane_groups, -(-classes // 8) * lane_groups
    left = first % axis_size + second % axis_size
    return second // axis_size, first // axis_size, -(-left // axis_size)


def piece_rows(feat_in, classes, hidden, axis_size):
    second, first, left = tile_counts(feat_in, classes, hidden, axis_size)
    sizes = [8 * second, 8 * (first // 2), 8 * (first - first // 2 + left)]
    return [(sum(sizes[:p]), size) for p, size in enumerate(sizes)]


def tile_places(feat_in, classes, hidden, axis_size):
    lane_groups = hidden // LANES
    second, first, left = tile_counts(feat_in, classes, hidden, axis_size)
    tiles = [[(owner, 8 * i, LANES * j) for i in range(-(-rows // 8)) for j in range(lane_groups)] for owner, rows in ((0, feat_in), (1, classes))]
    rest = tiles[0][first * axis_size:] + tiles[1][second * axis_size:]
    places = []
    for base, count, group in ((0, second, tiles[1]), (second, first, tiles[0]), (second + first, left, rest)):
        for i, tile in enumerate(group[:count * axis_size]):
            places.append((i % axis_size, 8 * (base + i // axis_size)) + tile)
    return places


def store_kernel(*refs):
    sources, targets, sems = refs[:3], refs[3:6], refs[6]
    copies = [pltpu.make_async_copy(src, dst, sems.at[i]) for i, (src, dst) in enumerate(zip(sources, targets))]
    for copy in copies:
        copy.start()
    for copy in copies:
        copy.wait()


def gcn_backward(axis_size, node_feats, a_int, a_halo, send_idx, w_first, w_second, grad_out):
    nodes, feat_in = node_feats.shape
    hidden, classes = w_second.shape
    links, slots = send_idx.shape
    halo = links * slots
    chips = axis_size // 2
    feat_pad = round_up(feat_in, 2 * LANES)
    feat_rows = round_up(feat_in, 16)
    class_pad = round_up(classes, LANES)
    class_rows = round_up(classes, 16)
    pieces = piece_rows(feat_in, classes, hidden, axis_size)
    assert chips == 8 and links == 4 and feat_in % 8 == 0
    chunk = (pieces[-1][0] + pieces[-1][1], LANES)
    vmem, dma = pltpu.VMEM, pltpu.SemaphoreType.DMA
    scratch = dict(
        featsT=vmem((feat_in, nodes), BF16), aint=vmem((nodes, nodes), BF16), ahalo=vmem((nodes, halo), BF16), idx=vmem((links, slots), jnp.int32),
        w1=vmem((feat_in, hidden), BF16), w2T=vmem((classes, hidden), BF16), gT=vmem((classes, nodes), BF16),
        featp=vmem((feat_pad, nodes), BF16), idxp=vmem((LANES, slots), F32), idxT=vmem((slots, LANES), F32), pick=vmem((2, nodes, slots), BF16), sel=vmem((halo, nodes), BF16),
        hsend=vmem((links, feat_rows, slots), BF16), hrecv=vmem((links, feat_pad, slots), BF16),
        pT=vmem((class_pad, nodes), F32), psend=vmem((links, class_rows, slots), BF16), precv=vmem((class_rows, halo), BF16),
        zf=vmem((nodes, feat_pad), F32), zb=vmem((nodes, feat_pad), BF16), zT=vmem((feat_pad, nodes), BF16),
        w1p=vmem((feat_rows, hidden), BF16), w1T=vmem((hidden, feat_pad), BF16), w2p=vmem((hidden, 2 * class_pad), BF16),
        h1T=vmem((hidden, nodes), BF16), fT=vmem((hidden, nodes), BF16), pairT=vmem((2 * class_pad, nodes), BF16), pair=vmem((nodes, 2 * class_pad), BF16),
        e0T=vmem((feat_rows, nodes), BF16), esend=vmem((links, feat_rows, slots), BF16), erecv=vmem((feat_rows, halo), BF16), gradT=vmem((feat_rows, nodes), F32),
        part=vmem((axis_size,) + chunk, F32), swap=vmem((chips,) + chunk, F32), mine=vmem((chips,) + chunk, F32), arbuf=vmem((7,) + chunk, F32), relay=vmem((2,) + chunk, F32), full=vmem((axis_size,) + chunk, F32),
        local_sem=dma((16,)), h_ssem=dma((links,)), h_rsem=dma((links,)), p_ssem=dma((links,)), p_rsem=dma((links,)), e_ssem=dma((links,)), e_rsem=dma((links,)), ar_ssem=dma((len(pieces), 23)), ar_rsem=dma((len(pieces), 23)))
    names = ["featsT_hbm", "aint_hbm", "ahalo_hbm", "idx_hbm", "w1_hbm", "w2T_hbm", "gT_hbm", "dw1", "dw2T", "gfT"] + list(scratch)
    any_spec = pl.BlockSpec(memory_space=pltpu.HBM)
    vmem_spec = pl.BlockSpec(memory_space=pltpu.VMEM)
    shapes = ((feat_in, hidden), (classes, hidden), (feat_in, nodes))
    sums = pl.pallas_call(
        functools.partial(gcn_kernel, axis_size, names),
        out_shape=tuple(pltpu.VMEM(shape, F32) for shape in shapes),
        in_specs=[any_spec] * 7,
        out_specs=(vmem_spec, vmem_spec, vmem_spec),
        scratch_shapes=list(scratch.values()),
        compiler_params=pltpu.CompilerParams(collective_id=0, has_side_effects=True, vmem_limit_bytes=VMEM_MIB * 1024 * 1024),
    )(*[pltpu.with_memory_space_constraint(x, pltpu.HBM) for x in (node_feats.T, a_int, a_halo, send_idx, w_first, w_second.T, grad_out.T)])
    dw_first, dw_second, grad_feats = pl.pallas_call(
        store_kernel,
        out_shape=tuple(jax.ShapeDtypeStruct(shape, F32) for shape in shapes),
        in_specs=[vmem_spec] * 3,
        out_specs=(any_spec,) * 3,
        scratch_shapes=[dma((3,))],
    )(*[pltpu.with_memory_space_constraint(x, pltpu.VMEM) for x in sums])
    return dw_first, dw_second.T, grad_feats.T


def solution(mesh):
    axis_size = mesh.shape["nodes"]
    row_spec = P(("graph", "nodes"), None)
    replicated = P(None, None)
    part_spec = P("graph", None)
    step = functools.partial(gcn_backward, axis_size)
    return jax.shard_map(step, mesh=mesh, in_specs=(row_spec, row_spec, row_spec, row_spec, replicated, replicated, row_spec), out_specs=(part_spec, part_spec, row_spec), check_vma=False)
```

```python
import functools

import jax
import jax.numpy as jnp
from jax import lax
from jax.experimental import pallas as pl
from jax.experimental.pallas import tpu as pltpu
from jax.sharding import PartitionSpec as P

BF16, F32 = jnp.bfloat16, jnp.float32
MESH = pl.DeviceIdType.MESH
LANES = 128
VMEM_MIB = 50


def link_offsets(num_links):
    return [(link // 2 + 1) * (1 - 2 * (link % 2)) for link in range(num_links)]


def round_up(size, unit):
    return -(-size // unit) * unit


def dot(left, right):
    return jnp.dot(left, right, preferred_element_type=F32)


def dot_lanes(left, right):
    return lax.dot_general(left, right, (((1,), (1,)), ((), ())), preferred_element_type=F32)


def pad_lanes(value, width):
    return jnp.concatenate([value, jnp.zeros((value.shape[0], width - value.shape[1]), value.dtype)], axis=1)


def pad_rows(value, height):
    return jnp.concatenate([value, jnp.zeros((height - value.shape[0], value.shape[1]), value.dtype)], axis=0)


def gcn_kernel(axis_size, names, *refs):
    r = dict(zip(names, refs, strict=True))
    featsT, aint, ahalo, idx, w1, w2T, gT = (r[k] for k in ("featsT", "aint", "ahalo", "idx", "w1", "w2T", "gT"))
    feat_in, nodes = featsT.shape
    classes, hidden = w2T.shape
    links, slots = idx.shape
    halo = links * slots
    offsets = link_offsets(links)
    feat_pad = r["featp"].shape[0]
    class_pad = r["pT"].shape[0]
    class_rows = r["precv"].shape[0]
    feat_rows = r["e0T"].shape[0]
    block = 512
    num_blocks = nodes // block
    me = lax.axis_index("nodes")
    chips = axis_size // 2
    core = me % 2
    sign = 1 - 2 * core
    chip = me // 2
    order = (2, 3, 0, 1)

    def at_offset(offset):
        return (me + offset + axis_size) % axis_size

    def remote(src, dst, send_sem, recv_sem, target):
        return pltpu.make_async_remote_copy(src_ref=src, dst_ref=dst, send_sem=send_sem, recv_sem=recv_sem, device_id={"nodes": target}, device_id_type=MESH)

    lsem = r["local_sem"]
    pairs = [(r["idx_hbm"], idx), (r["featsT_hbm"], featsT), (r["gT_hbm"], gT)]
    row_blocks = [pl.ds(b * block, block) for b in range(num_blocks)]
    pairs += [(r["ahalo_hbm"].at[rows], ahalo.at[rows]) for rows in row_blocks]
    pairs += [(r["w1_hbm"], w1), (r["w2T_hbm"], w2T)]
    pairs += [(r["aint_hbm"].at[rows], aint.at[rows]) for rows in row_blocks]
    copies = [pltpu.make_async_copy(src, dst, lsem.at[i]) for i, (src, dst) in enumerate(pairs)]
    for copy in copies[:5 + num_blocks]:
        copy.start()
    c_idx, c_feats, c_g = copies[:3]
    c_ahalo, (c_w1, c_w2), c_aint = copies[3:3 + num_blocks], copies[3 + num_blocks:5 + num_blocks], copies[5 + num_blocks:]

    barrier = pltpu.get_barrier_semaphore()
    peers = [1, -1, 2, -2]
    for offset in peers:
        pl.semaphore_signal(barrier, inc=1, device_id={"nodes": at_offset(offset)}, device_id_type=MESH)
    for k in range(links):
        r["hrecv"][k, feat_rows:feat_pad, :] = jnp.zeros((feat_pad - feat_rows, slots), BF16)

    c_idx.wait()
    pick, sel = r["pick"], r["sel"]
    sub = 16

    def fill_pick(buffer, k):
        index = idx[k:k + 1, :]
        low = jnp.broadcast_to(index % sub, (sub, slots))
        high = jnp.broadcast_to((index // sub).astype(F32), (sub, slots)).astype(BF16)
        ones = jnp.where(lax.broadcasted_iota(jnp.int32, (sub, slots), 0) == low, 1.0, 0.0).astype(BF16)
        zeros = jnp.zeros((sub, slots), BF16)
        cols = pl.ds((k % 2) * slots, slots)
        for m in range(nodes // sub):
            pick[buffer, m * sub:(m + 1) * sub, cols] = jnp.where(high == jnp.array(m, BF16), ones, zeros)

    def fill_sel(k):
        for i in range(slots // sub):
            col = jnp.broadcast_to(r["idxT"][i * sub:(i + 1) * sub, k:k + 1], (sub, LANES))
            tile = jnp.floor(col * (1.0 / LANES))
            lane = lax.broadcasted_iota(jnp.int32, (sub, LANES), 1).astype(F32)
            ones = jnp.where(lane == col - tile * LANES, 1.0, 0.0).astype(BF16)
            tile = tile.astype(BF16)
            row = k * slots + i * sub
            for t in range(nodes // LANES):
                sel[row:row + sub, t * LANES:(t + 1) * LANES] = jnp.where(tile == jnp.array(t, BF16), ones, jnp.zeros((sub, LANES), BF16))

    def both(buffer, value, first):
        buffer[first] = value[:, 0:slots]
        buffer[first + 1] = value[:, slots:2 * slots]

    hsends = {}

    def send_rows(first):
        for k in (first, first + 1):
            hsends[k] = remote(r["hsend"].at[k], r["hrecv"].at[k, pl.ds(0, feat_rows)], r["h_ssem"].at[k], r["h_rsem"].at[k], at_offset(offsets[k]))
            hsends[k].start()

    fill_pick(0, 2)
    fill_pick(0, 3)
    c_feats.wait()
    for copy in c_aint:
        copy.start()
    both(r["hsend"], pad_rows(dot(featsT[...], pick[0]), feat_rows).astype(BF16), 2)
    fill_pick(1, 0)
    fill_pick(1, 1)
    pl.semaphore_wait(barrier, len(peers))
    send_rows(2)
    both(r["hsend"], pad_rows(dot(featsT[...], pick[1]), feat_rows).astype(BF16), 0)
    r["idxp"][...] = jnp.zeros(r["idxp"].shape, F32)
    r["idxp"][0:links, :] = idx[...].astype(F32)
    r["idxT"][...] = r["idxp"][...].T
    send_rows(0)

    c_g.wait()
    for copy in c_ahalo:
        copy.wait()
    psends = {}
    for first in (2, 0):
        both(r["psend"], pad_rows(dot(gT[...], ahalo[:, first * slots:(first + 2) * slots]), class_rows).astype(BF16), first)
        fill_sel(first)
        fill_sel(first + 1)
        for k in (first, first + 1):
            cols = pl.ds(k * slots, slots)
            psends[k] = remote(r["psend"].at[k], r["precv"].at[:, cols], r["p_ssem"].at[k], r["p_rsem"].at[k], at_offset(-offsets[k]))
            psends[k].start()

    featp, pT = r["featp"], r["pT"]
    featp[...] = pad_rows(featsT[...], feat_pad)
    zf, zT, h1T = r["zf"], r["zT"], r["h1T"]
    for b in range(0, num_blocks, 2):
        c_aint[b].wait()
        c_aint[b + 1].wait()
        for rows in row_blocks[b:b + 2]:
            zf[rows, :] = dot_lanes(aint[rows, :], featp[...])
    c_w1.wait()
    c_w2.wait()
    w1p = r["w1p"]
    w1p[...] = pad_rows(w1[...], feat_rows)
    r["w1T"][...] = pad_rows(w1[...].astype(F32), feat_pad).T.astype(BF16)
    w2v = pad_rows(w2T[...].astype(F32), class_pad).T.astype(BF16)
    r["w2p"][...] = jnp.concatenate([w2v, w2v], axis=1)
    for b in range(num_blocks):
        cols = pl.ds(b * block, block)
        pT[:, cols] = pad_rows(dot(gT[...], aint[:, cols]), class_pad)

    for i, k in enumerate(order):
        cols = pl.ds(k * slots, slots)
        hsends[k].wait_recv()
        for b in range(num_blocks):
            rows = pl.ds(b * block, block)
            z = zf[rows, :] + dot_lanes(ahalo[rows, cols], r["hrecv"][k])
            if i < links - 1:
                zf[rows, :] = z
            else:
                zT[:, rows] = z.T.astype(BF16)
    for b in range(num_blocks):
        cols = pl.ds(b * block, block)
        h1T[:, cols] = jnp.maximum(dot(r["w1T"][...], zT[:, cols]), 0.0).astype(BF16)

    pairT = r["pairT"]
    for i, k in enumerate(order):
        slot = pl.ds(k * slots, slots)
        psends[k].wait_recv()
        for b in range(num_blocks):
            cols = pl.ds(b * block, block)
            total = pT[:, cols] + pad_rows(dot(r["precv"][:, slot], sel[slot, cols]), class_pad)
            if i < links - 1:
                pT[:, cols] = total
            else:
                high = total.astype(BF16)
                pairT[0:class_pad, cols] = high
                pairT[class_pad:2 * class_pad, cols] = (total - high.astype(F32)).astype(BF16)

    part, full = r["part"], r["full"]
    pieces = piece_rows(feat_in, classes, hidden, axis_size)
    places = tile_places(feat_in, classes, hidden, axis_size)
    half = core * chips
    other = (1 - core) * chips
    arsem_s, arsem_r = r["ar_ssem"], r["ar_rsem"]
    started = []

    def send(piece, slot, src, dst, target):
        copy = remote(src, dst, arsem_s.at[piece, slot], arsem_r.at[piece, slot], target)
        copy.start()
        started.append(copy)
        return copy

    def chip_at(distance):
        return (chip + distance * sign + 2 * chips) % chips

    def device_at(distance):
        return chip_at(distance) * 2 + core

    def rows_of(p):
        return pl.ds(pieces[p][0], pieces[p][1])

    sibling = me + sign
    mine, arbuf, relay = r["mine"], r["arbuf"], r["relay"]
    numbers = range(len(pieces))
    swap, first_step, second_step = {}, {}, {}

    def write_tiles(which, value):
        for q, row, owner, tile_row, lane in places:
            if owner == which:
                part[q, row:row + 8, :] = value[tile_row:tile_row + 8, lane:lane + LANES]

    def start_swap(p):
        swap[p] = send(p, 0, part.at[pl.ds(other, chips), rows_of(p)], r["swap"].at[:, rows_of(p)], sibling)

    def start_first(p):
        rows = rows_of(p)
        swap[p].wait_recv()
        mine[:, rows, :] = part[pl.ds(half, chips), rows, :] + r["swap"][:, rows, :]
        first_step[p] = [
            send(p, 2, mine.at[chip_at(4), rows], arbuf.at[1, rows], device_at(-2)),
            send(p, 1, mine.at[chip_at(-3), rows], arbuf.at[0, rows], device_at(-1)),
            send(p, 3, mine.at[chip_at(3), rows], arbuf.at[2, rows], device_at(1)),
            send(p, 4, mine.at[chip_at(-1), rows], arbuf.at[3, rows], device_at(-1)),
            send(p, 5, mine.at[chip_at(1), rows], arbuf.at[4, rows], device_at(1))]

    def start_second(p):
        rows = rows_of(p)
        c_a2, c_a1, c_b = first_step[p][:3]
        c_b.wait_recv()
        relay[1, rows, :] = mine[chip_at(2), rows, :] + arbuf[2, rows, :]
        c_em = send(p, 7, relay.at[1, rows], arbuf.at[6, rows], device_at(2))
        c_a1.wait_recv()
        c_a2.wait_recv()
        relay[0, rows, :] = mine[chip_at(-2), rows, :] + arbuf[0, rows, :] + arbuf[1, rows, :]
        c_ep = send(p, 6, relay.at[0, rows], arbuf.at[5, rows], device_at(-2))
        second_step[p] = [c_em, c_ep]

    fT = r["fT"]
    for b in range(num_blocks):
        cols = pl.ds(b * block, block)
        d1T = dot(r["w2p"][...], pairT[:, cols]).astype(BF16)
        fT[:, cols] = jnp.where(h1T[:, cols] > jnp.array(0, BF16), d1T, jnp.zeros_like(d1T))
    second, first = [], []
    for h in range(0, hidden, hidden // 2):
        rows = pl.ds(h, hidden // 2)
        value = dot_lanes(h1T[rows, :], pairT[...])
        second.append((value[:, 0:class_pad] + value[:, class_pad:2 * class_pad]).T)
        first.append(dot_lanes(fT[rows, :], zT[...]).T)
    write_tiles(1, jnp.concatenate(second, axis=1))
    write_tiles(0, jnp.concatenate(first, axis=1))
    for p in numbers:
        start_swap(p)

    e0T, gradT = r["e0T"], r["gradT"]
    for b in range(num_blocks):
        cols = pl.ds(b * block, block)
        e0T[:, cols] = dot(w1p[...], fT[:, cols]).astype(BF16)

    for p in numbers:
        start_first(p)
    for first in (2, 0):
        both(r["esend"], dot(e0T[...], ahalo[:, first * slots:(first + 2) * slots]).astype(BF16), first)
    esends = {}

    def send_back(first):
        for k in (first, first + 1):
            cols = pl.ds(k * slots, slots)
            esends[k] = remote(r["esend"].at[k], r["erecv"].at[:, cols], r["e_ssem"].at[k], r["e_rsem"].at[k], at_offset(-offsets[k]))
            esends[k].start()

    send_back(0)
    for b in range(num_blocks):
        cols = pl.ds(b * block, block)
        gradT[:, cols] = dot(e0T[...], aint[:, cols])
    for p in numbers:
        start_second(p)
    send_back(2)

    spreads = {}

    def spread(piece, slot, distance, target):
        place = full.at[half + chip_at(distance), rows_of(piece)]
        return send(piece, slot, place, place, target)

    def start_spread(p):
        rows = rows_of(p)
        for copy in first_step[p][3:] + second_step[p]:
            copy.wait_recv()
        full[half + chip, rows, :] = mine[chip, rows, :] + arbuf[3, rows, :] + arbuf[4, rows, :] + arbuf[5, rows, :] + arbuf[6, rows, :]
        spreads[p] = [spread(p, 10, 0, device_at(-2)), spread(p, 11, 0, device_at(2)), spread(p, 8, 0, device_at(-1)), spread(p, 9, 0, device_at(1)), spread(p, 15, 0, sibling)]

    for p in numbers:
        start_spread(p)

    for copy in esends.values():
        copy.wait_recv()
    for b in range(num_blocks):
        cols = pl.ds(b * block, block)
        total = gradT[:, cols] + dot(r["erecv"][...], sel[:, cols])
        r["gfT"][:, cols] = total[0:feat_in]

    lasts = []
    for p in numbers:
        g_p2, g_m2, g_p1, g_m1, to_sibling = spreads[p]
        g_p2.wait_recv()
        g_p4 = spread(p, 13, 2, device_at(-2))
        g_p3 = spread(p, 12, 2, device_at(-1))
        g_m2.wait_recv()
        g_m3 = spread(p, 14, -2, device_at(1))
        back = [to_sibling, spread(p, 16, 2, sibling), spread(p, 17, -2, sibling)]
        g_p1.wait_recv()
        back.append(spread(p, 18, 1, sibling))
        g_m1.wait_recv()
        back.append(spread(p, 19, -1, sibling))
        lasts.append([g_p3, g_m3, g_p4, back])
    for p in numbers:
        g_p3, g_m3, g_p4, back = lasts[p]
        g_p3.wait_recv()
        back.append(spread(p, 20, 3, sibling))
        g_m3.wait_recv()
        back.append(spread(p, 21, -3, sibling))
        g_p4.wait_recv()
        back.append(spread(p, 22, 4, sibling))
    for p in numbers:
        for copy in lasts[p][3]:
            copy.wait_recv()
    for q, row, owner, tile_row, lane in places:
        if owner == 0:
            r["dw1"][tile_row:tile_row + 8, lane:lane + LANES] = full[q, row:row + 8, :]
        elif owner == 1:
            count = min(8, classes - tile_row)
            r["dw2T"][tile_row:tile_row + count, lane:lane + LANES] = full[q, row:row + count, :]
    for copy in started + list(hsends.values()) + list(psends.values()) + list(esends.values()):
        copy.wait_send()


def tile_counts(feat_in, classes, hidden, axis_size):
    lane_groups = hidden // LANES
    first, second = -(-feat_in // 8) * lane_groups, -(-classes // 8) * lane_groups
    left = first % axis_size + second % axis_size
    return second // axis_size, first // axis_size, -(-left // axis_size)


def piece_rows(feat_in, classes, hidden, axis_size):
    second, first, left = tile_counts(feat_in, classes, hidden, axis_size)
    sizes = [8 * second, 8 * (first // 2), 8 * (first - first // 2 + left)]
    return [(sum(sizes[:p]), size) for p, size in enumerate(sizes)]


def tile_places(feat_in, classes, hidden, axis_size):
    lane_groups = hidden // LANES
    second, first, left = tile_counts(feat_in, classes, hidden, axis_size)
    tiles = [[(owner, 8 * i, LANES * j) for i in range(-(-rows // 8)) for j in range(lane_groups)] for owner, rows in ((0, feat_in), (1, classes))]
    rest = tiles[0][first * axis_size:] + tiles[1][second * axis_size:]
    places = []
    for base, count, group in ((0, second, tiles[1]), (second, first, tiles[0]), (second + first, left, rest)):
        for i, tile in enumerate(group[:count * axis_size]):
            places.append((i % axis_size, 8 * (base + i // axis_size)) + tile)
    return places


def store_kernel(*refs):
    sources, targets, sems = refs[:3], refs[3:6], refs[6]
    copies = [pltpu.make_async_copy(src, dst, sems.at[i]) for i, (src, dst) in enumerate(zip(sources, targets))]
    for copy in copies:
        copy.start()
    for copy in copies:
        copy.wait()


def gcn_backward(axis_size, node_feats, a_int, a_halo, send_idx, w_first, w_second, grad_out):
    nodes, feat_in = node_feats.shape
    hidden, classes = w_second.shape
    links, slots = send_idx.shape
    halo = links * slots
    chips = axis_size // 2
    feat_pad = round_up(feat_in, 2 * LANES)
    feat_rows = round_up(feat_in, 16)
    class_pad = round_up(classes, LANES)
    class_rows = round_up(classes, 16)
    pieces = piece_rows(feat_in, classes, hidden, axis_size)
    assert chips == 8 and links == 4 and feat_in % 8 == 0
    chunk = (pieces[-1][0] + pieces[-1][1], LANES)
    vmem, dma = pltpu.VMEM, pltpu.SemaphoreType.DMA
    scratch = dict(
        featsT=vmem((feat_in, nodes), BF16), aint=vmem((nodes, nodes), BF16), ahalo=vmem((nodes, halo), BF16), idx=vmem((links, slots), jnp.int32),
        w1=vmem((feat_in, hidden), BF16), w2T=vmem((classes, hidden), BF16), gT=vmem((classes, nodes), BF16),
        featp=vmem((feat_pad, nodes), BF16), idxp=vmem((LANES, slots), F32), idxT=vmem((slots, LANES), F32), pick=vmem((2, nodes, 2 * slots), BF16), sel=vmem((halo, nodes), BF16),
        hsend=vmem((links, feat_rows, slots), BF16), hrecv=vmem((links, feat_pad, slots), BF16),
        pT=vmem((class_pad, nodes), F32), psend=vmem((links, class_rows, slots), BF16), precv=vmem((class_rows, halo), BF16),
        zf=vmem((nodes, feat_pad), F32), zT=vmem((feat_pad, nodes), BF16),
        w1p=vmem((feat_rows, hidden), BF16), w1T=vmem((hidden, feat_pad), BF16), w2p=vmem((hidden, 2 * class_pad), BF16),
        h1T=vmem((hidden, nodes), BF16), fT=vmem((hidden, nodes), BF16), pairT=vmem((2 * class_pad, nodes), BF16),
        e0T=vmem((feat_rows, nodes), BF16), esend=vmem((links, feat_rows, slots), BF16), erecv=vmem((feat_rows, halo), BF16), gradT=vmem((feat_rows, nodes), F32),
        part=vmem((axis_size,) + chunk, F32), swap=vmem((chips,) + chunk, F32), mine=vmem((chips,) + chunk, F32), arbuf=vmem((7,) + chunk, F32), relay=vmem((2,) + chunk, F32), full=vmem((axis_size,) + chunk, F32),
        local_sem=dma((16,)), h_ssem=dma((links,)), h_rsem=dma((links,)), p_ssem=dma((links,)), p_rsem=dma((links,)), e_ssem=dma((links,)), e_rsem=dma((links,)), ar_ssem=dma((len(pieces), 23)), ar_rsem=dma((len(pieces), 23)))
    names = ["featsT_hbm", "aint_hbm", "ahalo_hbm", "idx_hbm", "w1_hbm", "w2T_hbm", "gT_hbm", "dw1", "dw2T", "gfT"] + list(scratch)
    any_spec = pl.BlockSpec(memory_space=pltpu.HBM)
    vmem_spec = pl.BlockSpec(memory_space=pltpu.VMEM)
    shapes = ((feat_in, hidden), (classes, hidden), (feat_in, nodes))
    sums = pl.pallas_call(
        functools.partial(gcn_kernel, axis_size, names),
        out_shape=tuple(pltpu.VMEM(shape, F32) for shape in shapes),
        in_specs=[any_spec] * 7,
        out_specs=(vmem_spec, vmem_spec, vmem_spec),
        scratch_shapes=list(scratch.values()),
        compiler_params=pltpu.CompilerParams(collective_id=0, has_side_effects=True, vmem_limit_bytes=VMEM_MIB * 1024 * 1024),
    )(*[pltpu.with_memory_space_constraint(x, pltpu.HBM) for x in (node_feats.T, a_int, a_halo, send_idx, w_first, w_second.T, grad_out.T)])
    dw_first, dw_second, grad_feats = pl.pallas_call(
        store_kernel,
        out_shape=tuple(jax.ShapeDtypeStruct(shape, F32) for shape in shapes),
        in_specs=[vmem_spec] * 3,
        out_specs=(any_spec,) * 3,
        scratch_shapes=[dma((3,))],
    )(*[pltpu.with_memory_space_constraint(x, pltpu.VMEM) for x in sums])
    return dw_first, dw_second.T, grad_feats.T


def solution(mesh):
    axis_size = mesh.shape["nodes"]
    row_spec = P(("graph", "nodes"), None)
    replicated = P(None, None)
    part_spec = P("graph", None)
    step = functools.partial(gcn_backward, axis_size)
    return jax.shard_map(step, mesh=mesh, in_specs=(row_spec, row_spec, row_spec, row_spec, replicated, replicated, row_spec), out_specs=(part_spec, part_spec, row_spec), check_vma=False)
```

```python
import functools

import jax
import jax.numpy as jnp
from jax import lax
from jax.experimental import pallas as pl
from jax.experimental.pallas import tpu as pltpu
from jax.sharding import PartitionSpec as P

BF16, F32 = jnp.bfloat16, jnp.float32
MESH = pl.DeviceIdType.MESH
LANES = 128
VMEM_MIB = 50


def link_offsets(num_links):
    return [(link // 2 + 1) * (1 - 2 * (link % 2)) for link in range(num_links)]


def round_up(size, unit):
    return -(-size // unit) * unit


def dot(left, right):
    return jnp.dot(left, right, preferred_element_type=F32)


def dot_lanes(left, right):
    return lax.dot_general(left, right, (((1,), (1,)), ((), ())), preferred_element_type=F32)


def pad_lanes(value, width):
    return jnp.concatenate([value, jnp.zeros((value.shape[0], width - value.shape[1]), value.dtype)], axis=1)


def pad_rows(value, height):
    return jnp.concatenate([value, jnp.zeros((height - value.shape[0], value.shape[1]), value.dtype)], axis=0)


def gcn_kernel(axis_size, names, *refs):
    r = dict(zip(names, refs, strict=True))
    featsT, aint, ahalo, idx, w1, w2T, gT = (r[k] for k in ("featsT", "aint", "ahalo", "idx", "w1", "w2T", "gT"))
    feat_in, nodes = featsT.shape
    classes, hidden = w2T.shape
    links, slots = idx.shape
    halo = links * slots
    offsets = link_offsets(links)
    feat_pad = r["featp"].shape[0]
    class_pad = r["pT"].shape[0]
    class_rows = r["precv"].shape[0]
    feat_rows = r["e0T"].shape[0]
    block = 512
    num_blocks = nodes // block
    me = lax.axis_index("nodes")
    chips = axis_size // 2
    core = me % 2
    sign = 1 - 2 * core
    chip = me // 2
    order = (2, 3, 0, 1)

    def at_offset(offset):
        return (me + offset + axis_size) % axis_size

    def remote(src, dst, send_sem, recv_sem, target):
        return pltpu.make_async_remote_copy(src_ref=src, dst_ref=dst, send_sem=send_sem, recv_sem=recv_sem, device_id={"nodes": target}, device_id_type=MESH)

    lsem = r["local_sem"]
    pairs = [(r["idx_hbm"], idx), (r["featsT_hbm"], featsT), (r["gT_hbm"], gT)]
    row_blocks = [pl.ds(b * block, block) for b in range(num_blocks)]
    pairs += [(r["ahalo_hbm"].at[rows], ahalo.at[rows]) for rows in row_blocks]
    pairs += [(r["w1_hbm"], w1), (r["w2T_hbm"], w2T)]
    pairs += [(r["aint_hbm"].at[rows], aint.at[rows]) for rows in row_blocks]
    copies = [pltpu.make_async_copy(src, dst, lsem.at[i]) for i, (src, dst) in enumerate(pairs)]
    for copy in copies[:5 + num_blocks]:
        copy.start()
    c_idx, c_feats, c_g = copies[:3]
    c_ahalo, (c_w1, c_w2), c_aint = copies[3:3 + num_blocks], copies[3 + num_blocks:5 + num_blocks], copies[5 + num_blocks:]

    barrier = pltpu.get_barrier_semaphore()
    peers = [1, -1, 2, -2]
    for offset in peers:
        pl.semaphore_signal(barrier, inc=1, device_id={"nodes": at_offset(offset)}, device_id_type=MESH)
    r["hrecv"][feat_rows:feat_pad, :] = jnp.zeros((feat_pad - feat_rows, halo), BF16)

    c_idx.wait()
    pick, sel = r["pick"], r["sel"]
    sub = 16

    def fill_pick(buffer, k):
        index = idx[k:k + 1, :]
        low = jnp.broadcast_to(index % sub, (sub, slots))
        high = jnp.broadcast_to((index // sub).astype(F32), (sub, slots)).astype(BF16)
        ones = jnp.where(lax.broadcasted_iota(jnp.int32, (sub, slots), 0) == low, 1.0, 0.0).astype(BF16)
        zeros = jnp.zeros((sub, slots), BF16)
        cols = pl.ds((k % 2) * slots, slots)
        for m in range(nodes // sub):
            pick[buffer, m * sub:(m + 1) * sub, cols] = jnp.where(high == jnp.array(m, BF16), ones, zeros)

    def fill_sel(k):
        for i in range(slots // sub):
            col = jnp.broadcast_to(r["idxT"][i * sub:(i + 1) * sub, k:k + 1], (sub, LANES))
            tile = jnp.floor(col * (1.0 / LANES))
            lane = lax.broadcasted_iota(jnp.int32, (sub, LANES), 1).astype(F32)
            ones = jnp.where(lane == col - tile * LANES, 1.0, 0.0).astype(BF16)
            tile = tile.astype(BF16)
            row = k * slots + i * sub
            for t in range(nodes // LANES):
                sel[row:row + sub, t * LANES:(t + 1) * LANES] = jnp.where(tile == jnp.array(t, BF16), ones, jnp.zeros((sub, LANES), BF16))

    def both(buffer, value, first):
        buffer[first] = value[:, 0:slots]
        buffer[first + 1] = value[:, slots:2 * slots]

    hsends = {}

    def send_rows(first):
        for k in (first, first + 1):
            hsends[k] = remote(r["hsend"].at[k], r["hrecv"].at[pl.ds(0, feat_rows), pl.ds(k * slots, slots)], r["h_ssem"].at[k], r["h_rsem"].at[k], at_offset(offsets[k]))
            hsends[k].start()

    fill_pick(0, 2)
    fill_pick(0, 3)
    c_feats.wait()
    for copy in c_aint:
        copy.start()
    both(r["hsend"], pad_rows(dot(featsT[...], pick[0]), feat_rows).astype(BF16), 2)
    fill_pick(1, 0)
    fill_pick(1, 1)
    pl.semaphore_wait(barrier, len(peers))
    send_rows(2)
    both(r["hsend"], pad_rows(dot(featsT[...], pick[1]), feat_rows).astype(BF16), 0)
    r["idxp"][...] = jnp.zeros(r["idxp"].shape, F32)
    r["idxp"][0:links, :] = idx[...].astype(F32)
    r["idxT"][...] = r["idxp"][...].T
    send_rows(0)

    c_g.wait()
    for copy in c_ahalo:
        copy.wait()
    psends = {}
    for first in (2, 0):
        both(r["psend"], pad_rows(dot(gT[...], ahalo[:, first * slots:(first + 2) * slots]), class_rows).astype(BF16), first)
        for k in (first, first + 1):
            cols = pl.ds(k * slots, slots)
            psends[k] = remote(r["psend"].at[k], r["precv"].at[:, cols], r["p_ssem"].at[k], r["p_rsem"].at[k], at_offset(-offsets[k]))
            psends[k].start()

    featp, pT = r["featp"], r["pT"]
    featp[...] = pad_rows(featsT[...], feat_pad)
    zf, zT, h1T = r["zf"], r["zT"], r["h1T"]
    for b in range(0, num_blocks, 2):
        c_aint[b].wait()
        c_aint[b + 1].wait()
        for rows in row_blocks[b:b + 2]:
            zf[rows, :] = dot_lanes(aint[rows, :], featp[...])
        fill_sel(b)
        fill_sel(b + 1)
    c_w1.wait()
    c_w2.wait()
    w1p = r["w1p"]
    w1p[...] = pad_rows(w1[...], feat_rows)
    r["w1T"][...] = pad_rows(w1[...].astype(F32), feat_pad).T.astype(BF16)
    w2v = pad_rows(w2T[...].astype(F32), class_pad).T.astype(BF16)
    r["w2p"][...] = jnp.concatenate([w2v, w2v], axis=1)
    for b in range(num_blocks):
        cols = pl.ds(b * block, block)
        pT[:, cols] = pad_rows(dot(gT[...], aint[:, cols]), class_pad)

    for first in (2, 0):
        cols = pl.ds(first * slots, 2 * slots)
        for k in (first, first + 1):
            hsends[k].wait_recv()
        for b in range(num_blocks):
            rows = pl.ds(b * block, block)
            z = zf[rows, :] + dot_lanes(ahalo[rows, cols], r["hrecv"][:, cols])
            if first:
                zf[rows, :] = z
            else:
                zT[:, rows] = z.T.astype(BF16)
    for b in range(num_blocks):
        cols = pl.ds(b * block, block)
        h1T[:, cols] = jnp.maximum(dot(r["w1T"][...], zT[:, cols]), 0.0).astype(BF16)

    pairT = r["pairT"]
    for k in order:
        psends[k].wait_recv()
    for b in range(num_blocks):
        cols = pl.ds(b * block, block)
        total = pT[:, cols] + pad_rows(dot(r["precv"][...], sel[:, cols]), class_pad)
        high = total.astype(BF16)
        pairT[0:class_pad, cols] = high
        pairT[class_pad:2 * class_pad, cols] = (total - high.astype(F32)).astype(BF16)

    part, full = r["part"], r["full"]
    pieces = piece_rows(feat_in, classes, hidden, axis_size)
    places = tile_places(feat_in, classes, hidden, axis_size)
    half = core * chips
    other = (1 - core) * chips
    arsem_s, arsem_r = r["ar_ssem"], r["ar_rsem"]
    started = []

    def send(piece, slot, src, dst, target):
        copy = remote(src, dst, arsem_s.at[piece, slot], arsem_r.at[piece, slot], target)
        copy.start()
        started.append(copy)
        return copy

    def chip_at(distance):
        return (chip + distance * sign + 2 * chips) % chips

    def device_at(distance):
        return chip_at(distance) * 2 + core

    def across(distance):
        return chip_at(distance) * 2 + 1 - core

    def rows_of(p):
        return pl.ds(pieces[p][0], pieces[p][1])

    sibling = me + sign
    mine, arbuf, relay = r["mine"], r["arbuf"], r["relay"]
    numbers = range(len(pieces))
    swap, first_step, second_step = {}, {}, {}

    def write_tiles(which, value, lane0):
        for q, row, owner, tile_row, lane in places:
            if owner == which and lane0 <= lane < lane0 + value.shape[1]:
                part[q, row:row + 8, :] = value[tile_row:tile_row + 8, lane - lane0:lane - lane0 + LANES]

    def start_swap(p):
        swap[p] = send(p, 0, part.at[pl.ds(other, chips), rows_of(p)], r["swap"].at[:, rows_of(p)], sibling)

    def start_first(p):
        rows = rows_of(p)
        swap[p].wait_recv()
        mine[:, rows, :] = part[pl.ds(half, chips), rows, :] + r["swap"][:, rows, :]
        first_step[p] = [
            send(p, 2, mine.at[chip_at(4), rows], arbuf.at[1, rows], device_at(-2)),
            send(p, 1, mine.at[chip_at(-3), rows], arbuf.at[0, rows], device_at(-1)),
            send(p, 3, mine.at[chip_at(3), rows], arbuf.at[2, rows], device_at(1)),
            send(p, 4, mine.at[chip_at(-1), rows], arbuf.at[3, rows], device_at(-1)),
            send(p, 5, mine.at[chip_at(1), rows], arbuf.at[4, rows], device_at(1))]

    def start_second(p):
        rows = rows_of(p)
        c_a2, c_a1, c_b = first_step[p][:3]
        c_b.wait_recv()
        relay[1, rows, :] = mine[chip_at(2), rows, :] + arbuf[2, rows, :]
        c_em = send(p, 7, relay.at[1, rows], arbuf.at[6, rows], device_at(2))
        c_a1.wait_recv()
        c_a2.wait_recv()
        relay[0, rows, :] = mine[chip_at(-2), rows, :] + arbuf[0, rows, :] + arbuf[1, rows, :]
        c_ep = send(p, 6, relay.at[0, rows], arbuf.at[5, rows], device_at(-2))
        second_step[p] = [c_em, c_ep]

    fT = r["fT"]
    for h in range(2):
        rows = pl.ds(h * (hidden // 2), hidden // 2)
        for b in range(num_blocks):
            cols = pl.ds(b * block, block)
            d1T = dot(r["w2p"][rows, :], pairT[:, cols]).astype(BF16)
            fT[rows, cols] = jnp.where(h1T[rows, cols] > jnp.array(0, BF16), d1T, jnp.zeros_like(d1T))
        value = dot_lanes(h1T[rows, :], pairT[...])
        write_tiles(1, (value[:, 0:class_pad] + value[:, class_pad:2 * class_pad]).T, h * (hidden // 2))
        write_tiles(0, dot_lanes(fT[rows, :], zT[...]).T, h * (hidden // 2))
        if h == 0:
            start_swap(0)
        else:
            start_first(0)
            for p in numbers[1:]:
                start_swap(p)

    e0T, gradT = r["e0T"], r["gradT"]
    for b in range(num_blocks):
        cols = pl.ds(b * block, block)
        e0T[:, cols] = dot(w1p[...], fT[:, cols]).astype(BF16)

    for p in numbers[1:]:
        start_first(p)
    for first in (2, 0):
        both(r["esend"], dot(e0T[...], ahalo[:, first * slots:(first + 2) * slots]).astype(BF16), first)
    esends = {}

    def send_back(first):
        for k in (first, first + 1):
            cols = pl.ds(k * slots, slots)
            esends[k] = remote(r["esend"].at[k], r["erecv"].at[:, cols], r["e_ssem"].at[k], r["e_rsem"].at[k], at_offset(-offsets[k]))
            esends[k].start()

    send_back(0)
    for b in range(num_blocks):
        cols = pl.ds(b * block, block)
        gradT[:, cols] = dot(e0T[...], aint[:, cols])
    for p in numbers:
        start_second(p)
    send_back(2)

    spreads = {}

    def spread(piece, slot, distance, target):
        place = full.at[half + chip_at(distance), rows_of(piece)]
        return send(piece, slot, place, place, target)

    def start_spread(p):
        rows = rows_of(p)
        for copy in first_step[p][3:] + second_step[p]:
            copy.wait_recv()
        full[half + chip, rows, :] = mine[chip, rows, :] + arbuf[3, rows, :] + arbuf[4, rows, :] + arbuf[5, rows, :] + arbuf[6, rows, :]
        spreads[p] = [spread(p, 10, 0, device_at(-2)), spread(p, 11, 0, device_at(2)), spread(p, 8, 0, device_at(-1)), spread(p, 9, 0, device_at(1)), spread(p, 15, 0, sibling)]

    for p in numbers:
        start_spread(p)

    for copy in esends.values():
        copy.wait_recv()
    for b in range(num_blocks):
        cols = pl.ds(b * block, block)
        total = gradT[:, cols] + dot(r["erecv"][...], sel[:, cols])
        r["gfT"][:, cols] = total[0:feat_in]

    lasts = []
    for p in numbers:
        g_p2, g_m2, g_p1, g_m1, to_sibling = spreads[p]
        g_p2.wait_recv()
        over = [spread(p, 13, 2, device_at(-2)), spread(p, 22, 2, across(-2)), spread(p, 12, 2, device_at(-1)), spread(p, 20, 2, across(-1))]
        g_m2.wait_recv()
        over += [spread(p, 14, -2, device_at(1)), spread(p, 21, -2, across(1))]
        back = [to_sibling, spread(p, 16, 2, sibling), spread(p, 17, -2, sibling)]
        g_p1.wait_recv()
        back.append(spread(p, 18, 1, sibling))
        g_m1.wait_recv()
        back.append(spread(p, 19, -1, sibling))
        lasts.append(back + over)
    for p in numbers:
        for copy in lasts[p]:
            copy.wait_recv()
    for q, row, owner, tile_row, lane in places:
        if owner == 0:
            r["dw1"][tile_row:tile_row + 8, lane:lane + LANES] = full[q, row:row + 8, :]
        elif owner == 1:
            count = min(8, classes - tile_row)
            r["dw2T"][tile_row:tile_row + count, lane:lane + LANES] = full[q, row:row + count, :]
    for copy in started + list(hsends.values()) + list(psends.values()) + list(esends.values()):
        copy.wait_send()


def tile_count(feat_in, classes, hidden, axis_size):
    tiles = (-(-feat_in // 8) - (-classes // 8)) * (hidden // LANES // 2)
    return -(-tiles // axis_size)


def piece_rows(feat_in, classes, hidden, axis_size):
    count = tile_count(feat_in, classes, hidden, axis_size)
    sizes = [8 * count, 8 * (count - count // 2), 8 * (count // 2)]
    return [(sum(sizes[:p]), size) for p, size in enumerate(sizes)]


def tile_places(feat_in, classes, hidden, axis_size):
    count = tile_count(feat_in, classes, hidden, axis_size)
    groups = hidden // LANES // 2
    places = []
    for h in range(2):
        tiles = [(owner, 8 * i, LANES * (h * groups + j)) for owner, rows in ((1, classes), (0, feat_in)) for i in range(-(-rows // 8)) for j in range(groups)]
        places += [(i % axis_size, 8 * (h * count + i // axis_size)) + tile for i, tile in enumerate(tiles)]
    return places


def store_kernel(*refs):
    sources, targets, sems = refs[:3], refs[3:6], refs[6]
    copies = [pltpu.make_async_copy(src, dst, sems.at[i]) for i, (src, dst) in enumerate(zip(sources, targets))]
    for copy in copies:
        copy.start()
    for copy in copies:
        copy.wait()


def gcn_backward(axis_size, node_feats, a_int, a_halo, send_idx, w_first, w_second, grad_out):
    nodes, feat_in = node_feats.shape
    hidden, classes = w_second.shape
    links, slots = send_idx.shape
    halo = links * slots
    chips = axis_size // 2
    feat_pad = round_up(feat_in, 2 * LANES)
    feat_rows = round_up(feat_in, 16)
    class_pad = round_up(classes, LANES)
    class_rows = round_up(classes, 16)
    pieces = piece_rows(feat_in, classes, hidden, axis_size)
    assert chips == 8 and links == 4 and feat_in % 8 == 0
    chunk = (pieces[-1][0] + pieces[-1][1], LANES)
    vmem, dma = pltpu.VMEM, pltpu.SemaphoreType.DMA
    scratch = dict(
        featsT=vmem((feat_in, nodes), BF16), aint=vmem((nodes, nodes), BF16), ahalo=vmem((nodes, halo), BF16), idx=vmem((links, slots), jnp.int32),
        w1=vmem((feat_in, hidden), BF16), w2T=vmem((classes, hidden), BF16), gT=vmem((classes, nodes), BF16),
        featp=vmem((feat_pad, nodes), BF16), idxp=vmem((LANES, slots), F32), idxT=vmem((slots, LANES), F32), pick=vmem((2, nodes, 2 * slots), BF16), sel=vmem((halo, nodes), BF16),
        hsend=vmem((links, feat_rows, slots), BF16), hrecv=vmem((feat_pad, halo), BF16),
        pT=vmem((class_pad, nodes), F32), psend=vmem((links, class_rows, slots), BF16), precv=vmem((class_rows, halo), BF16),
        zf=vmem((nodes, feat_pad), F32), zT=vmem((feat_pad, nodes), BF16),
        w1p=vmem((feat_rows, hidden), BF16), w1T=vmem((hidden, feat_pad), BF16), w2p=vmem((hidden, 2 * class_pad), BF16),
        h1T=vmem((hidden, nodes), BF16), fT=vmem((hidden, nodes), BF16), pairT=vmem((2 * class_pad, nodes), BF16),
        e0T=vmem((feat_rows, nodes), BF16), esend=vmem((links, feat_rows, slots), BF16), erecv=vmem((feat_rows, halo), BF16), gradT=vmem((feat_rows, nodes), F32),
        part=vmem((axis_size,) + chunk, F32), swap=vmem((chips,) + chunk, F32), mine=vmem((chips,) + chunk, F32), arbuf=vmem((7,) + chunk, F32), relay=vmem((2,) + chunk, F32), full=vmem((axis_size,) + chunk, F32),
        local_sem=dma((16,)), h_ssem=dma((links,)), h_rsem=dma((links,)), p_ssem=dma((links,)), p_rsem=dma((links,)), e_ssem=dma((links,)), e_rsem=dma((links,)), ar_ssem=dma((len(pieces), 23)), ar_rsem=dma((len(pieces), 23)))
    names = ["featsT_hbm", "aint_hbm", "ahalo_hbm", "idx_hbm", "w1_hbm", "w2T_hbm", "gT_hbm", "dw1", "dw2T", "gfT"] + list(scratch)
    any_spec = pl.BlockSpec(memory_space=pltpu.HBM)
    vmem_spec = pl.BlockSpec(memory_space=pltpu.VMEM)
    shapes = ((feat_in, hidden), (classes, hidden), (feat_in, nodes))
    sums = pl.pallas_call(
        functools.partial(gcn_kernel, axis_size, names),
        out_shape=tuple(pltpu.VMEM(shape, F32) for shape in shapes),
        in_specs=[any_spec] * 7,
        out_specs=(vmem_spec, vmem_spec, vmem_spec),
        scratch_shapes=list(scratch.values()),
        compiler_params=pltpu.CompilerParams(collective_id=0, has_side_effects=True, vmem_limit_bytes=VMEM_MIB * 1024 * 1024),
    )(*[pltpu.with_memory_space_constraint(x, pltpu.HBM) for x in (node_feats.T, a_int, a_halo, send_idx, w_first, w_second.T, grad_out.T)])
    dw_first, dw_second, grad_feats = pl.pallas_call(
        store_kernel,
        out_shape=tuple(jax.ShapeDtypeStruct(shape, F32) for shape in shapes),
        in_specs=[vmem_spec] * 3,
        out_specs=(any_spec,) * 3,
        scratch_shapes=[dma((3,))],
    )(*[pltpu.with_memory_space_constraint(x, pltpu.VMEM) for x in sums])
    return dw_first, dw_second.T, grad_feats.T


def solution(mesh):
    axis_size = mesh.shape["nodes"]
    row_spec = P(("graph", "nodes"), None)
    replicated = P(None, None)
    part_spec = P("graph", None)
    step = functools.partial(gcn_backward, axis_size)
    return jax.shard_map(step, mesh=mesh, in_specs=(row_spec, row_spec, row_spec, row_spec, replicated, replicated, row_spec), out_specs=(part_spec, part_spec, row_spec), check_vma=False)
```
